32 devices in a mesh: ctx: 4 (over z), head: 8 (over y, x, core).
Axes of the slice: x: 2, y: 2, z: 4, core: 2. Of those that a mesh axis runs over, the one named last changes fastest.
Arguments:
- video: bfloat16 [3072, 4096], P('ctx', 'head'), may hold values from -6 to 6
- audio: bfloat16 [384, 2048], P('ctx', 'head'), may hold values from -6 to 6
- video_gain: float32 [4096], P('head'), may hold values from 0.1 to 1.9
- audio_gain: float32 [2048], P('head'), may hold values from 0.1 to 1.9
- video_qkv: bfloat16 [4096, 3, 4096], P(None, None, 'head'), as said below
- video_cross: bfloat16 [4096, 3, 2048], P(None, None, 'head'), as said below
- audio_cross: bfloat16 [2048, 3, 2048], P(None, None, 'head'), as said below
- video_out: bfloat16 [4096, 4096], P('head'), may hold values from -0.09375 to 0.09375
- cross_video_out: bfloat16 [2048, 4096], P('head'), may hold values from -0.125 to 0.125
- cross_audio_out: bfloat16 [2048, 2048], P('head'), may hold values from -0.125 to 0.125
Outputs:
- video_result: bfloat16 [3072, 4096], P('ctx', 'head')
- audio_result: bfloat16 [384, 2048], P('ctx', 'head')
The draws below stay inside these ranges and needn't reach their ends.
Inputs may be any that keep to these rules, and one draw needn't show every extreme that they name: `video_qkv`: entries lie within -32 / sqrt(4096) and 32 / sqrt(4096). `video_cross`: entries lie within -32 / sqrt(4096) and 32 / sqrt(4096). `audio_cross`: entries lie within -32 / sqrt(2048) and 32 / sqrt(2048).
All inputs are finite; a program needn't handle non-finite values.
Results may differ from the reference program's by a relative error of at most 0.014.
The reference program's roundings to bfloat16 on the way count: a program that leaves them out, or rounds other values in their place, can miss the bound.
Values may be sent and summed in bfloat16 or wider, within the bound.
A program may use at most 128 MiB of HBM per device.

```python
import jax
import jax.numpy as jnp
from jax import lax

DV = 4096
DA = 2048
DC = 2048
HD = 128
VTOK = 3072
ATOK = 384


def projection_draw(key, element_salt, heads_salt, rows, width):
    element_key = jax.random.fold_in(key, element_salt)
    heads = width // HD
    flags = (jax.random.permutation(jax.random.fold_in(key, heads_salt), heads) < max(1, heads // 4)).astype(jnp.float32)
    factor = 8.0
    base = jax.random.truncated_normal(element_key, -4.0, 4.0, (rows, 3, width), jnp.float32)
    columns = jnp.repeat(1.0 + (factor - 1.0) * flags, HD)
    blocks = jnp.array([1.0, 1.0, 0.0], jnp.float32)
    scaling = 1.0 + blocks[:, None] * (columns[None, :] - 1.0)
    return (base * scaling[None, :, :] * rows ** (-0.5)).astype(jnp.bfloat16)


def draw_video_qkv(key, part):
    return projection_draw(key, 11, 21, DV, DV)


def draw_video_cross(key, part):
    return projection_draw(key, 12, 22, DV, DC)


def draw_audio_cross(key, part):
    return projection_draw(key, 13, 22, DA, DC)


def level_of(own_key, shape, pieces, low, largest):
    loudness = 1.0
    for dim, shards_of in pieces:
        draws = jax.random.uniform(jax.random.fold_in(jax.random.fold_in(own_key, 6), dim), (shards_of,), jnp.float32, low / len(pieces), largest / len(pieces))
        loudness = loudness * jnp.repeat(jnp.exp(draws), shape[dim] // shards_of).reshape((-1,) + (1,) * (len(shape) - 1 - dim))
    return loudness


def bell_draw(own_key, dims, scale, most, pieces=(), held_as=jnp.bfloat16):
    values = scale * jax.random.normal(own_key, dims, jnp.float32)
    if pieces:
        values = values * level_of(own_key, dims, pieces, -0.22, 0.18)
    return jnp.clip(values, -most, most).astype(held_as)


def setup_inputs(seed: int = 0) -> dict:
    key_list = jax.random.split(jax.random.key(seed), 11)
    video = bell_draw(key_list[0], (VTOK, DV), 1.0, 6.0, ((0, 4), (1, 8)))
    audio = bell_draw(key_list[1], (ATOK, DA), 1.0, 6.0, ((0, 4), (1, 8)))
    video_gain = jnp.clip(1.0 + 0.18 * jax.random.normal(key_list[2], (DV,), jnp.float32), 0.1, 1.9)
    audio_gain = jnp.clip(1.0 + 0.18 * jax.random.normal(key_list[3], (DA,), jnp.float32), 0.1, 1.9)
    video_qkv = draw_video_qkv(jax.random.fold_in(key_list[10], 71), 0)
    video_cross = draw_video_cross(jax.random.fold_in(key_list[10], 71), 0)
    audio_cross = draw_audio_cross(jax.random.fold_in(key_list[10], 71), 0)
    video_out = bell_draw(key_list[7], (DV, DV), DV ** -0.5, 0.09375, ((0, 8),))
    cross_video_out = bell_draw(key_list[8], (DC, DV), DC ** -0.5, 0.125, ((0, 8),))
    cross_audio_out = bell_draw(key_list[9], (DC, DA), DC ** -0.5, 0.125, ((0, 8),))
    return dict(video=video, audio=audio, video_gain=video_gain, audio_gain=audio_gain, video_qkv=video_qkv, video_cross=video_cross, audio_cross=audio_cross, video_out=video_out, cross_video_out=cross_video_out, cross_audio_out=cross_audio_out)


EPSILON = 1e-06

def attend(queries, keys, values):
    heads = queries.shape[1] // HD
    scale = HD ** (-0.5)

    def split_heads(matrix):
        return matrix.reshape(matrix.shape[0], heads, HD).transpose(1, 0, 2)

    def one_head(operands):
        query_block, key_block, value_block = operands
        scores = jnp.dot(query_block, key_block.T, preferred_element_type=jnp.float32) * scale
        highest = lax.optimization_barrier(jnp.max(scores, axis=1, keepdims=True))
        weights = jnp.exp(scores - highest)
        totals = lax.optimization_barrier(jnp.sum(weights, axis=1, keepdims=True))
        return jnp.dot(weights.astype(jnp.bfloat16), value_block, preferred_element_type=jnp.float32) / totals
    blocks = lax.map(one_head, (split_heads(queries), split_heads(keys), split_heads(values)))
    return blocks.transpose(1, 0, 2).reshape(queries.shape[0], heads * HD).astype(jnp.bfloat16)

def reference(video, audio, video_gain, audio_gain, video_qkv, video_cross, audio_cross, video_out, cross_video_out, cross_audio_out):
    video_wide = video.astype(jnp.float32)
    audio_wide = audio.astype(jnp.float32)
    video_rate = lax.rsqrt(lax.optimization_barrier(jnp.sum(video_wide * video_wide, axis=1)) / DV + EPSILON)
    audio_rate = lax.rsqrt(lax.optimization_barrier(jnp.sum(audio_wide * audio_wide, axis=1)) / DA + EPSILON)
    video_scaled = (video_wide * video_gain).astype(jnp.bfloat16)
    audio_scaled = (audio_wide * audio_gain).astype(jnp.bfloat16)
    self_proj = (jnp.dot(video_scaled, video_qkv.reshape(DV, 3 * DV), preferred_element_type=jnp.float32) * video_rate[:, None]).astype(jnp.bfloat16)
    video_mixed = (jnp.dot(video_scaled, video_cross.reshape(DV, 3 * DC), preferred_element_type=jnp.float32) * video_rate[:, None]).astype(jnp.bfloat16)
    audio_mixed = (jnp.dot(audio_scaled, audio_cross.reshape(DA, 3 * DC), preferred_element_type=jnp.float32) * audio_rate[:, None]).astype(jnp.bfloat16)
    self_out = attend(self_proj[:, :DV], self_proj[:, DV:2 * DV], self_proj[:, 2 * DV:])
    video_cross_out = attend(video_mixed[:, :DC], audio_mixed[:, DC:2 * DC], audio_mixed[:, 2 * DC:])
    audio_cross_out = attend(audio_mixed[:, :DC], video_mixed[:, DC:2 * DC], video_mixed[:, 2 * DC:])
    video_sum = jnp.dot(self_out, video_out, preferred_element_type=jnp.float32) + jnp.dot(video_cross_out, cross_video_out, preferred_element_type=jnp.float32)
    audio_sum = jnp.dot(audio_cross_out, cross_audio_out, preferred_element_type=jnp.float32)
    return ((video_wide + video_sum).astype(jnp.bfloat16), (audio_wide + audio_sum).astype(jnp.bfloat16))
```

```python
import functools
import math

import jax
import jax.numpy as jnp
from jax import lax
from jax.experimental import pallas as pl
from jax.experimental.pallas import tpu as pltpu

from jax.sharding import PartitionSpec as P

HD = 128


EPSILON = 1e-06


def split_heads(matrix):
    return matrix.reshape(matrix.shape[0], -1, HD).transpose(1, 0, 2)


def join_heads(blocks):
    return blocks.transpose(1, 0, 2).reshape(blocks.shape[1], -1)


def attend(queries, keys, values):
    scale = HD ** (-0.5)

    def one_head(operands):
        query_block, key_block, value_block = operands
        scores = jnp.dot(query_block, key_block.T, preferred_element_type=jnp.float32) * scale
        highest = jnp.max(scores, axis=1, keepdims=True)
        weights = jnp.exp(scores - highest)
        totals = jnp.sum(weights, axis=1, keepdims=True)
        return (
            jnp.dot(weights.astype(jnp.bfloat16), value_block, preferred_element_type=jnp.float32)
            / totals
        )

    blocks = lax.map(one_head, (split_heads(queries), split_heads(keys), split_heads(values)))
    return join_heads(blocks).astype(jnp.bfloat16)


def plain_body(
    video,
    audio,
    video_gain,
    audio_gain,
    video_qkv,
    video_cross,
    audio_cross,
    video_out,
    cross_video_out,
    cross_audio_out,
):
    scale = HD ** (-0.5)
    video_wide = video.astype(jnp.float32)
    audio_wide = audio.astype(jnp.float32)
    video_squares, audio_squares = lax.psum(
        (jnp.sum(video_wide * video_wide, axis=1), jnp.sum(audio_wide * audio_wide, axis=1)), "head"
    )
    video_rate = lax.rsqrt(video_squares / video_qkv.shape[0] + EPSILON)
    audio_rate = lax.rsqrt(audio_squares / audio_cross.shape[0] + EPSILON)
    video_scaled = (video_wide * video_gain).astype(jnp.bfloat16)
    audio_scaled = (audio_wide * audio_gain).astype(jnp.bfloat16)
    self_weight = video_qkv.reshape(video_qkv.shape[0], -1)
    mixed_weight = video_cross.reshape(video_cross.shape[0], -1)
    audio_weight = audio_cross.reshape(audio_cross.shape[0], -1)
    self_width = video_qkv.shape[2]
    cross_width = video_cross.shape[2]
    video_rows = video.shape[0]
    segment = lax.all_gather(video_scaled, "head", axis=1, tiled=True)
    self_acc = jnp.dot(segment, self_weight, preferred_element_type=jnp.float32)
    mixed_acc = jnp.dot(segment, mixed_weight, preferred_element_type=jnp.float32)
    audio_acc = jnp.dot(
        lax.all_gather(audio_scaled, "head", axis=1, tiled=True),
        audio_weight,
        preferred_element_type=jnp.float32,
    )
    self_proj = (self_acc * video_rate[:, None]).astype(jnp.bfloat16)
    video_mixed = (mixed_acc * video_rate[:, None]).astype(jnp.bfloat16)
    audio_mixed = (audio_acc * audio_rate[:, None]).astype(jnp.bfloat16)
    query_heads = split_heads(self_proj[:, :self_width])
    local_heads = query_heads.shape[0]
    running_max = jnp.full((local_heads, video_rows), -1e30, jnp.float32)
    key_heads = split_heads(
        lax.all_gather(self_proj[:, self_width : 2 * self_width], "ctx", axis=0, tiled=True)
    )
    value_heads = split_heads(
        lax.all_gather(self_proj[:, 2 * self_width :], "ctx", axis=0, tiled=True)
    )
    scores = (
        jnp.einsum("hqd,hkd->hqk", query_heads, key_heads, preferred_element_type=jnp.float32)
        * scale
    )
    newest = jnp.maximum(running_max, jnp.max(scores, axis=2))
    weights = jnp.exp(scores - newest[:, :, None])
    running_sum = jnp.sum(weights, axis=2)
    running_acc = jnp.einsum(
        "hqk,hkd->hqd",
        weights.astype(jnp.bfloat16),
        value_heads,
        preferred_element_type=jnp.float32,
    )
    self_out = join_heads(running_acc / running_sum[:, :, None]).astype(jnp.bfloat16)
    audio_key_all, audio_value_all = (
        lax.all_gather(audio_mixed[:, cross_width : 2 * cross_width], "ctx", axis=0, tiled=True),
        lax.all_gather(audio_mixed[:, 2 * cross_width :], "ctx", axis=0, tiled=True),
    )
    video_cross_out = attend(video_mixed[:, :cross_width], audio_key_all, audio_value_all)
    queries_av = audio_mixed[:, :cross_width]
    keys_av = video_mixed[:, cross_width : 2 * cross_width]
    values_av = video_mixed[:, 2 * cross_width :]
    every_query = lax.all_gather(queries_av, "ctx", axis=0, tiled=True)
    scores = (
        jnp.einsum(
            "hqd,hkd->hqk",
            split_heads(every_query),
            split_heads(keys_av),
            preferred_element_type=jnp.float32,
        )
        * scale
    )
    highest = lax.pmax(jnp.max(scores, axis=2), "ctx")
    weights = jnp.exp(scores - highest[:, :, None])
    numerators = jnp.einsum(
        "hqk,hkd->hqd",
        weights.astype(jnp.bfloat16),
        split_heads(values_av),
        preferred_element_type=jnp.float32,
    )
    weight_totals = jnp.sum(weights, axis=2)
    own_numer, own_totals = (
        lax.psum_scatter(
            numerators.astype(jnp.bfloat16), "ctx", scatter_dimension=1, tiled=True
        ).astype(jnp.float32),
        lax.psum_scatter(
            weight_totals.astype(jnp.bfloat16), "ctx", scatter_dimension=1, tiled=True
        ).astype(jnp.float32),
    )
    audio_cross_out = join_heads(own_numer / own_totals[:, :, None]).astype(jnp.bfloat16)
    video_partial = jnp.dot(self_out, video_out, preferred_element_type=jnp.float32) + jnp.dot(
        video_cross_out, cross_video_out, preferred_element_type=jnp.float32
    )
    audio_partial = jnp.dot(audio_cross_out, cross_audio_out, preferred_element_type=jnp.float32)
    video_sum, audio_sum = (
        lax.psum_scatter(
            video_partial.astype(jnp.bfloat16), "head", scatter_dimension=1, tiled=True
        ).astype(jnp.float32),
        lax.psum_scatter(
            audio_partial.astype(jnp.bfloat16), "head", scatter_dimension=1, tiled=True
        ).astype(jnp.float32),
    )
    return (
        (video_wide + video_sum).astype(jnp.bfloat16),
        (audio_wide + audio_sum).astype(jnp.bfloat16),
    )


MESH = pl.DeviceIdType.MESH
F32 = jnp.float32
BF16 = jnp.bfloat16
VMEM_LIMIT = 62 * 1024 * 1024
CHUNK = HD
SCORE_SCALE = HD ** (-0.5) * math.log2(math.e)


def head_peer(me, flip):
    low = me % 2
    mid = (me // 2) % 2
    high = me // 4
    if flip & 1:
        low = 1 - low
    if flip & 2:
        mid = 1 - mid
    if flip & 4:
        high = 1 - high
    return high * 4 + mid * 2 + low


def remote(source, target, send, recv, device):
    return pltpu.make_async_remote_copy(
        src_ref=source,
        dst_ref=target,
        send_sem=send,
        recv_sem=recv,
        device_id=device,
        device_id_type=MESH,
    )


def diagonal(rows):
    line = lax.broadcasted_iota(jnp.int32, (rows, HD), 0)
    lane = lax.broadcasted_iota(jnp.int32, (rows, HD), 1)
    return line == lane


def to_row(column):
    rows = column.shape[0]
    spread = jnp.broadcast_to(column, (rows, HD))
    return jnp.sum(jnp.where(diagonal(rows), spread, 0.0), axis=0, keepdims=True)


def to_column(row, rows):
    spread = jnp.broadcast_to(row, (rows, HD))
    return jnp.sum(jnp.where(diagonal(rows), spread, 0.0), axis=1, keepdims=True)


def contract_last(left, right):
    return lax.dot_general(left, right, (((1,), (1,)), ((), ())), preferred_element_type=F32)


def softmax_parts(query, keys, values):
    scores = [contract_last(query, key) for key in keys]
    highest = functools.reduce(
        jnp.maximum, [jnp.max(score, axis=1, keepdims=True) for score in scores]
    )
    total = 0.0
    mixed = 0.0
    for score, value in zip(scores, values):
        weight = jnp.exp2((score - highest) * SCORE_SCALE)
        total = total + jnp.sum(weight, axis=1, keepdims=True)
        mixed = mixed + jnp.dot(weight.astype(BF16), value, preferred_element_type=F32)
    return mixed, total, highest * SCORE_SCALE


def aligned(start, size):
    return pl.ds(pl.multiple_of(start, size), size)


def entry_kernel(
    ctx_size,
    video_ref,
    audio_ref,
    video_gain_ref,
    audio_gain_ref,
    w_self_ref,
    w_cross_ref,
    w_audio_ref,
    source_ref,
    cross_out_ref,
    sound_ref,
    xs,
    xa,
    squares,
    every_square,
    w_self,
    w_cross,
    w_audio,
    heads,
    cross,
    tones,
    parts,
    parts_in,
    stats,
    stats_in,
    load,
    plane_send,
    plane_recv,
    tone_send,
    tone_recv,
    square_send,
    square_recv,
    key_send,
    key_recv,
    late_send,
    late_recv,
):
    ctx = lax.axis_index("ctx")
    me = lax.axis_index("head")
    rows, width = video_ref.shape
    audio_rows, audio_width = audio_ref.shape
    count = rows // CHUNK
    local_heads = width // HD
    cross_width = w_cross.shape[2]
    cross_heads = cross_width // HD
    peer = [head_peer(me, flip) for flip in range(8)]
    mates = [(ctx + d) % ctx_size for d in range(ctx_size)]

    plane_order = (1, 2, 0)
    loads = {}
    for i, plane in enumerate(plane_order):
        loads[plane] = pltpu.make_async_copy(w_self_ref.at[plane], w_self.at[plane], load.at[i])
        loads[plane].start()
    load_audio = pltpu.make_async_copy(w_audio_ref, w_audio, load.at[3])
    load_cross = pltpu.make_async_copy(w_cross_ref, w_cross, load.at[4])
    load_audio.start()
    load_cross.start()

    barrier = pltpu.get_barrier_semaphore()
    friends = [(ctx, peer[flip]) for flip in range(1, 8)]
    friends += [(mates[d], me) for d in range(1, ctx_size)]
    for friend in friends:
        pl.semaphore_signal(barrier, inc=1, device_id=friend, device_id_type=MESH)

    def at_rows(k):
        return aligned(k * CHUNK, CHUNK)

    def columns(block):
        return aligned(block * width, width)

    def tone_columns(block):
        return aligned(block * audio_width, audio_width)

    for k in range(count):
        wide = video_ref[pl.ds(k * CHUNK, CHUNK)].astype(F32)
        xs[pl.ds(k * CHUNK, CHUNK), columns(me)] = (wide * video_gain_ref[...]).astype(BF16)
        squares[k : k + 1] = to_row(jnp.sum(wide * wide, axis=1, keepdims=True))
    wide = audio_ref[...].astype(F32)
    xa[:, tone_columns(me)] = (wide * audio_gain_ref[...]).astype(BF16)
    squares[count : count + 1] = to_row(jnp.sum(wide * wide, axis=1, keepdims=True))
    every_square[0] = squares[...]

    pl.semaphore_wait(barrier, len(friends))

    def hop(slot, k, flip, block):
        part = xs.at[at_rows(k), columns(block)]
        return remote(part, part, plane_send.at[slot, k], plane_recv.at[slot, k], (ctx, peer[flip]))

    def tone_hop(slot, flip, block):
        part = xa.at[:, tone_columns(block)]
        return remote(part, part, tone_send.at[slot], tone_recv.at[slot], (ctx, peer[flip]))

    def direct_x(k):
        return hop(0, k, 2, me)

    def direct_y(k):
        return hop(1, k, 4, me)

    def side(k):
        return hop(2, k, 1, me)

    def far(k, parity):
        return hop(3, k, 2, peer[4]) if parity else hop(3, k, 4, peer[2])

    def side_x(k):
        return hop(4, k, 1, peer[2])

    def side_y(k):
        return hop(5, k, 1, peer[4])

    def side_far(k):
        return hop(6, k, 1, peer[6])

    tone_hops = [
        tone_hop(0, 2, me),
        tone_hop(1, 4, me),
        tone_hop(2, 1, me),
        tone_hop(3, 4, peer[2]),
        tone_hop(4, 1, peer[2]),
        tone_hop(5, 1, peer[4]),
        tone_hop(6, 1, peer[6]),
    ]
    square_hops = [
        remote(
            squares,
            every_square.at[flip],
            square_send.at[flip - 1],
            square_recv.at[flip - 1],
            (ctx, peer[flip]),
        )
        for flip in range(1, 8)
    ]

    def begin(k):
        direct_x(k).start()
        direct_y(k).start()
        side(k).start()

    begin(0)
    for one in square_hops:
        one.start()
    for one in tone_hops[:3]:
        one.start()
    begin(1)

    def spread(k, parity, more):
        direct_x(k).wait_recv()
        if parity == 0:
            far(k, parity).start()
        side_x(k).start()
        direct_y(k).wait_recv()
        if parity == 1:
            far(k, parity).start()
        side_y(k).start()
        if more:
            begin(k + 2)

    def key_copy(k, d):
        return remote(
            heads.at[mates[d], pl.ds(1, 2), at_rows(k)],
            source_ref.at[ctx, pl.ds(1, 2), at_rows(k)],
            key_send.at[d - 1, k],
            key_recv.at[d - 1, k],
            (mates[d], me),
        )

    def late_copy(kind, d):
        source, target = {
            0: (heads.at[mates[d], 0], source_ref.at[ctx, 0]),
            1: (
                tones.at[aligned(ctx * audio_rows, audio_rows)],
                tones.at[aligned(ctx * audio_rows, audio_rows)],
            ),
            2: (parts.at[mates[d]], parts_in.at[ctx]),
            3: (stats.at[mates[d]], stats_in.at[ctx]),
        }[kind]
        return remote(
            source, target, late_send.at[kind, d - 1], late_recv.at[kind, d - 1], (mates[d], me)
        )

    def video_rate(k):
        sums = jnp.sum(every_square[:, pl.ds(k, 1), :], axis=0)
        return to_column(lax.rsqrt(sums / (8 * width) + EPSILON), CHUNK)

    def project(k):
        at = at_rows(k)
        side(k).wait_recv()
        side_x(k).wait_recv()
        side_y(k).wait_recv()
        side_far(k).wait_recv()
        rate = video_rate(k)

        def one(i, carry):
            plane = (i + 1) % 3
            acc = jnp.dot(xs[at, :], w_self[plane], preferred_element_type=F32)
            scaled = (acc * rate).astype(BF16)
            for h in range(local_heads):
                heads[h, plane, at] = scaled[:, h * HD : (h + 1) * HD]
            return carry

        lax.fori_loop(0, 2, one, 0)
        for d in range(1, ctx_size):
            key_copy(k, d).start()
        lax.fori_loop(2, 3, one, 0)
        for plane in range(3):
            source_ref[ctx, plane, at] = heads[ctx, plane, at]

        def other(plane, carry):
            acc = jnp.dot(xs[at, :], w_cross[plane], preferred_element_type=F32)
            scaled = (acc * rate).astype(BF16)
            for h in range(cross_heads):
                cross[h, plane, at] = scaled[:, h * HD : (h + 1) * HD]
            return carry

        lax.fori_loop(0, 3, other, 0)

    def advance(k, parity, more):
        @pl.when(k + 1 < count)
        def _():
            spread(k + 1, 1 - parity, False)

            @pl.when(k + 3 < count)
            def _():
                begin(k + 3)

        far(k, parity).wait_recv()
        side_far(k).start()
        project(k)

    spread(0, 0, True)
    for one in square_hops:
        one.wait_recv()
    loads[1].wait()
    loads[2].wait()
    loads[0].wait()
    load_cross.wait()

    def sing():
        tone_hops[0].wait_recv()
        tone_hops[3].start()
        tone_hops[4].start()
        tone_hops[1].wait_recv()
        tone_hops[5].start()
        load_audio.wait()
        sums = jnp.sum(every_square[:, count : count + 1, :], axis=0)
        rate = to_column(lax.rsqrt(sums / (8 * audio_width) + EPSILON), audio_rows)
        tone_hops[3].wait_recv()
        tone_hops[6].start()
        for slot in (2, 4, 5, 6):
            tone_hops[slot].wait_recv()
        at = aligned(ctx * audio_rows, audio_rows)
        for plane in range(3):
            acc = jnp.dot(xa[...], w_audio[plane], preferred_element_type=F32)
            tones[at, plane * cross_width : (plane + 1) * cross_width] = (acc * rate).astype(BF16)
        for d in range(1, ctx_size):
            late_copy(1, d).start()

    advance(0, 0, True)
    sing()
    advance(1, 1, True)

    def two(i, carry):
        advance(2 * i, 0, True)
        advance(2 * i + 1, 1, True)
        return carry

    lax.fori_loop(1, count // 2, two, 0)
    for d in range(1, ctx_size):
        late_copy(0, d).start()

    for d in range(1, ctx_size):
        late_copy(1, d).wait_recv()
    sound_tile = math.gcd(rows, 256)
    for h in range(cross_heads):
        at = [
            slice(plane * cross_width + h * HD, plane * cross_width + (h + 1) * HD)
            for plane in range(3)
        ]
        own = slice(h * HD, (h + 1) * HD)

        def answer(d, carry):
            query = tones[aligned(d * audio_rows, audio_rows), at[0]]
            mixed, total, highest = softmax_parts(query, [cross[h, 1]], [cross[h, 2]])
            parts[d, :, own] = (mixed / total).astype(BF16)
            stats[d, 2 * h : 2 * h + 1] = to_row(total)
            stats[d, 2 * h + 1 : 2 * h + 2] = to_row(highest)
            return carry

        lax.fori_loop(0, ctx_size, answer, 0)
    for d in range(1, ctx_size):
        late_copy(2, d).start()
        late_copy(3, d).start()
    parts_in[ctx] = parts[ctx]
    stats_in[ctx] = stats[ctx]
    for h in range(cross_heads):
        at = [
            slice(plane * cross_width + h * HD, plane * cross_width + (h + 1) * HD)
            for plane in range(3)
        ]
        own = slice(h * HD, (h + 1) * HD)

        def ask(i, carry):
            tile = aligned(i * sound_tile, sound_tile)
            mixed, total, _ = softmax_parts(cross[h, 0, tile], [tones[:, at[1]]], [tones[:, at[2]]])
            cross_out_ref[tile, own] = (mixed / total).astype(BF16)
            return carry

        lax.fori_loop(0, rows // sound_tile, ask, 0)

    for d in range(1, ctx_size):
        late_copy(2, d).wait_recv()
        late_copy(3, d).wait_recv()
    for h in range(cross_heads):
        own = slice(h * HD, (h + 1) * HD)
        totals = [stats_in[s, 2 * h : 2 * h + 1] for s in range(ctx_size)]
        highs = [stats_in[s, 2 * h + 1 : 2 * h + 2] for s in range(ctx_size)]
        top = functools.reduce(jnp.maximum, highs)
        shares = [total * jnp.exp2(high - top) for total, high in zip(totals, highs)]
        whole = functools.reduce(jnp.add, shares)
        mixed = 0.0
        for s in range(ctx_size):
            share = to_column(shares[s] / whole, audio_rows)
            mixed = mixed + parts_in[s, :, own].astype(F32) * share
        sound_ref[:, own] = mixed.astype(BF16)

    def finish(k, carry):
        for d in range(1, ctx_size):
            key_copy(k, d).wait()
        direct_x(k).wait_send()
        direct_y(k).wait_send()
        for one in (side(k), far(k, 0), side_x(k), side_y(k), side_far(k)):
            one.wait_send()
        return carry

    lax.fori_loop(0, count, finish, 0)
    for d in range(1, ctx_size):
        late_copy(0, d).wait()
        for kind in (1, 2, 3):
            late_copy(kind, d).wait_send()
    for one in tone_hops + square_hops:
        one.wait_send()


def entry(ctx_size, video, audio, video_gain, audio_gain, video_qkv, video_cross, audio_cross):
    rows, width = video.shape
    audio_rows, audio_width = audio.shape
    depth = video_qkv.shape[0]
    audio_depth = audio_cross.shape[0]
    cross_width = video_cross.shape[2]
    count = rows // CHUNK
    local_heads = width // HD
    cross_heads = cross_width // HD
    lines = (count + 1 + 7) // 8 * 8
    vmem = pl.BlockSpec(memory_space=pltpu.VMEM)
    anywhere = pl.BlockSpec(memory_space=pl.ANY)
    dma = pltpu.SemaphoreType.DMA
    others = ctx_size - 1
    return pl.pallas_call(
        functools.partial(entry_kernel, ctx_size),
        out_shape=(
            jax.ShapeDtypeStruct((ctx_size, 3, rows, HD), BF16),
            jax.ShapeDtypeStruct((rows, cross_width), BF16),
            jax.ShapeDtypeStruct((audio_rows, cross_width), BF16),
        ),
        in_specs=[vmem] * 4 + [anywhere] * 3,
        out_specs=(vmem, vmem, vmem),
        scratch_shapes=[
            pltpu.VMEM((rows, depth), BF16),
            pltpu.VMEM((audio_rows, audio_depth), BF16),
            pltpu.VMEM((lines, HD), F32),
            pltpu.VMEM((8, lines, HD), F32),
            pltpu.VMEM((3, depth, width), BF16),
            pltpu.VMEM((3, depth, cross_width), BF16),
            pltpu.VMEM((3, audio_depth, cross_width), BF16),
            pltpu.VMEM((local_heads, 3, rows, HD), BF16),
            pltpu.VMEM((cross_heads, 3, rows, HD), BF16),
            pltpu.VMEM((ctx_size * audio_rows, 3 * cross_width), BF16),
            pltpu.VMEM((ctx_size, audio_rows, cross_width), BF16),
            pltpu.VMEM((ctx_size, audio_rows, cross_width), BF16),
            pltpu.VMEM((ctx_size, 8, HD), F32),
            pltpu.VMEM((ctx_size, 8, HD), F32),
            dma((5,)),
            dma((7, count)),
            dma((7, count)),
            dma((7,)),
            dma((7,)),
            dma((7,)),
            dma((7,)),
            dma((others, count)),
            dma((others, count)),
            dma((4, others)),
            dma((4, others)),
        ],
        compiler_params=pltpu.CompilerParams(
            collective_id=0, has_side_effects=True, vmem_limit_bytes=VMEM_LIMIT
        ),
        name="entry",
    )(
        video,
        audio,
        video_gain.reshape(1, -1),
        audio_gain.reshape(1, -1),
        video_qkv.transpose(1, 0, 2),
        video_cross.transpose(1, 0, 2),
        audio_cross.transpose(1, 0, 2),
    )


def exit_kernel(
    ctx_size,
    source_ref,
    cross_ref,
    sound_ref,
    video_ref,
    audio_ref,
    w_self_ref,
    w_cross_ref,
    w_audio_ref,
    video_out_ref,
    audio_out_ref,
    w_self,
    w_cross,
    w_audio,
    own,
    mixed_out,
    part,
    chip,
    landed,
    tone_part,
    tone_chip,
    tone_landed,
    load,
    back_send,
    back_recv,
    side_send,
    side_recv,
    hop_send,
    hop_recv,
    tone_send,
    tone_recv,
):
    ctx = lax.axis_index("ctx")
    me = lax.axis_index("head")
    rows, width = video_ref.shape
    count = rows // CHUNK
    peer = [head_peer(me, flip) for flip in range(8)]
    mates = [(ctx + d) % ctx_size for d in range(ctx_size)]
    load_audio = pltpu.make_async_copy(w_audio_ref, w_audio, load.at[0])
    load_self = pltpu.make_async_copy(w_self_ref, w_self, load.at[1])
    load_cross = pltpu.make_async_copy(w_cross_ref, w_cross, load.at[2])
    for one in (load_audio, load_self, load_cross):
        one.start()
    barrier = pltpu.get_barrier_semaphore()
    friends = [(ctx, peer[flip]) for flip in (1, 2, 4)]
    friends += [(mates[d], me) for d in range(1, ctx_size)]
    for friend in friends:
        pl.semaphore_signal(barrier, inc=1, device_id=friend, device_id_type=MESH)

    def at_rows(k):
        return aligned(k * CHUNK, CHUNK)

    def reducer(part, chip, landed, at, sems, out_ref, base_ref, parity):
        side_sems, hop_sems = sems
        near_flip, end_flip = (4, 2) if parity else (2, 4)
        near, end = near_flip // 2, end_flip // 2

        def side(i):
            return remote(
                part.at[peer[2 * i + 1], at], chip.at[i, at], *side_sems(i), (ctx, peer[1])
            )

        def hop(slot, flip, k):
            return remote(chip.at[k, at], landed.at[slot, at], *hop_sems(slot), (ctx, peer[flip]))

        def far_hop():
            return hop(0, near_flip, 3)

        def near_hop():
            return hop(1, near_flip, near)

        def end_hop():
            return hop(2, end_flip, end)

        def start():
            for i in (3, near, end, 0):
                side(i).start()

        def fold(i):
            side(i).wait_recv()
            chip[i, at] = (chip[i, at].astype(F32) + part[peer[2 * i], at].astype(F32)).astype(BF16)

        def join():
            fold(3)
            far_hop().start()
            fold(near)
            near_hop().start()
            fold(end)

        def pass_on():
            far_hop().wait_recv()
            chip[end, at] = (chip[end, at].astype(F32) + landed[0, at].astype(F32)).astype(BF16)
            end_hop().start()

        def close():
            side(0).wait_recv()
            total = chip[0, at].astype(F32) + part[me, at].astype(F32) + base_ref[at].astype(F32)
            near_hop().wait_recv()
            total = total + landed[1, at].astype(F32)
            end_hop().wait_recv()
            out_ref[at] = (total + landed[2, at].astype(F32)).astype(BF16)

        def settle():
            for i in range(4):
                side(i).wait_send()
            for one in (far_hop(), near_hop(), end_hop()):
                one.wait_send()

        return start, join, pass_on, close, settle

    def video_steps(k, parity):
        sems = (
            lambda i: (side_send.at[i, k], side_recv.at[i, k]),
            lambda slot: (hop_send.at[slot, k], hop_recv.at[slot, k]),
        )
        return reducer(part, chip, landed, at_rows(k), sems, video_out_ref, video_ref, parity)

    tone_steps = reducer(
        tone_part,
        tone_chip,
        tone_landed,
        pl.ds(0, audio_ref.shape[0]),
        (
            lambda i: (tone_send.at[i], tone_recv.at[i]),
            lambda slot: (tone_send.at[4 + slot], tone_recv.at[4 + slot]),
        ),
        audio_out_ref,
        audio_ref,
        0,
    )

    load_audio.wait()
    tone_width = audio_ref.shape[1]
    for n in range(8):
        tone_part[n] = jnp.dot(
            sound_ref[...],
            w_audio[:, n * tone_width : (n + 1) * tone_width],
            preferred_element_type=F32,
        ).astype(BF16)
    pl.semaphore_wait(barrier, len(friends))
    tone_steps[0]()

    def back(k, d):
        return remote(
            own.at[mates[d], at_rows(k)],
            mixed_out.at[ctx, at_rows(k)],
            back_send.at[d - 1, k],
            back_recv.at[d - 1, k],
            (mates[d], me),
        )

    keys = [source_ref.at[s, 1] for s in range(ctx_size)]
    values = [source_ref.at[s, 2] for s in range(ctx_size)]

    def attend_pair(k, first):
        at = at_rows(k)
        pair = [mates[(first + i) % ctx_size] for i in range(2)]
        query = jnp.concatenate([source_ref[s, 0, at] for s in pair], axis=0)
        mixed, total, _ = softmax_parts(
            query, [key[...] for key in keys], [value[...] for value in values]
        )
        done = (mixed / total).astype(BF16)
        for i, s in enumerate(pair):
            own[s, at] = done[i * CHUNK : (i + 1) * CHUNK]
            d = (first + i) % ctx_size
            if d:
                back(k, d).start()
            else:
                mixed_out[ctx, at] = done[i * CHUNK : (i + 1) * CHUNK]

    def output(k):
        at = at_rows(k)
        for d in range(1, ctx_size):
            back(k, d).wait_recv()
        selfs = jnp.concatenate([mixed_out[s, at] for s in range(ctx_size)], axis=1)

        def one(n, carry):
            cols = aligned(n * width, width)
            part[n, at] = (
                jnp.dot(selfs, w_self[:, cols], preferred_element_type=F32)
                + jnp.dot(cross_ref[at], w_cross[:, cols], preferred_element_type=F32)
            ).astype(BF16)
            return carry

        lax.fori_loop(0, 8, one, 0)
        video_steps(k, 0)[0]()

    def turn(k, parity):
        attend_pair(k, 1)

        @pl.when(k >= 2)
        def _():
            video_steps(k - 2, parity)[2]()

        @pl.when(k >= 1)
        def _():
            output(k - 1)

        attend_pair(k, 3)

        @pl.when(k >= 1)
        def _():
            video_steps(k - 1, 1 - parity)[1]()

        @pl.when(k >= 3)
        def _():
            video_steps(k - 3, 1 - parity)[3]()

    def two(i, carry):
        turn(2 * i, 0)

        @pl.when(i == 0)
        def _():
            tone_steps[1]()
            load_self.wait()
            load_cross.wait()

        turn(2 * i + 1, 1)

        @pl.when(i == 0)
        def _():
            tone_steps[2]()

        return carry

    lax.fori_loop(0, count // 2, two, 0)
    last = count - 1
    video_steps(last - 1, 0)[2]()
    output(last)
    video_steps(last, 1)[1]()
    tone_steps[3]()
    video_steps(last - 2, 1)[3]()
    video_steps(last - 1, 0)[3]()
    video_steps(last, 1)[2]()
    video_steps(last, 1)[3]()

    def finish(k, carry):
        for d in range(1, ctx_size):
            back(k, d).wait_send()
        video_steps(k, 0)[4]()
        return carry

    lax.fori_loop(0, count, finish, 0)
    tone_steps[4]()


def leave(ctx_size, sources, cross_out, sound, video, audio, w_self, w_cross, w_audio):
    rows, width = video.shape
    audio_rows, audio_width = audio.shape
    count = rows // CHUNK
    vmem = pl.BlockSpec(memory_space=pltpu.VMEM)
    anywhere = pl.BlockSpec(memory_space=pl.ANY)
    dma = pltpu.SemaphoreType.DMA
    others = ctx_size - 1
    return pl.pallas_call(
        functools.partial(exit_kernel, ctx_size),
        out_shape=(
            jax.ShapeDtypeStruct(video.shape, BF16),
            jax.ShapeDtypeStruct(audio.shape, BF16),
        ),
        in_specs=[vmem] * 5 + [anywhere] * 3,
        out_specs=(vmem, vmem),
        scratch_shapes=[
            pltpu.VMEM(w_self.shape, BF16),
            pltpu.VMEM(w_cross.shape, BF16),
            pltpu.VMEM(w_audio.shape, BF16),
            pltpu.VMEM((ctx_size, rows, HD), BF16),
            pltpu.VMEM((ctx_size, rows, HD), BF16),
            pltpu.VMEM((8, rows, width), BF16),
            pltpu.VMEM((4, rows, width), BF16),
            pltpu.VMEM((3, rows, width), BF16),
            pltpu.VMEM((8, audio_rows, audio_width), BF16),
            pltpu.VMEM((4, audio_rows, audio_width), BF16),
            pltpu.VMEM((3, audio_rows, audio_width), BF16),
            dma((3,)),
            dma((others, count)),
            dma((others, count)),
            dma((4, count)),
            dma((4, count)),
            dma((3, count)),
            dma((3, count)),
            dma((7,)),
            dma((7,)),
        ],
        compiler_params=pltpu.CompilerParams(
            collective_id=1, has_side_effects=True, vmem_limit_bytes=VMEM_LIMIT
        ),
        name="leave",
    )(sources, cross_out, sound, video, audio, w_self, w_cross, w_audio)


def fast_body(
    ctx_size,
    video,
    audio,
    video_gain,
    audio_gain,
    video_qkv,
    video_cross,
    audio_cross,
    video_out,
    cross_video_out,
    cross_audio_out,
):
    sources, cross_out, sound = entry(
        ctx_size, video, audio, video_gain, audio_gain, video_qkv, video_cross, audio_cross
    )
    return leave(
        ctx_size,
        sources,
        cross_out,
        sound,
        video,
        audio,
        video_out,
        cross_video_out,
        cross_audio_out,
    )


def suits(ctx_size, head_size, video, audio, video_cross):
    rows, width = video.shape
    audio_rows, audio_width = audio.shape
    return (
        head_size == 8
        and ctx_size == 4
        and width == ctx_size * HD
        and rows % (2 * CHUNK) == 0
        and rows >= 4 * CHUNK
        and audio_rows % 16 == 0
        and audio_rows <= HD
        and audio_width % HD == 0
        and video_cross.shape[2] % HD == 0
        and video_cross.shape[2] <= 4 * HD
    )


def solution(mesh):
    ctx_size = mesh.shape["ctx"]

    def body(*operands):
        if suits(ctx_size, mesh.shape["head"], operands[0], operands[1], operands[5]):
            return fast_body(ctx_size, *operands)
        return plain_body(*operands)

    return jax.shard_map(
        body,
        mesh=mesh,
        in_specs=(
            P("ctx", "head"),
            P("ctx", "head"),
            P("head"),
            P("head"),
            P(None, None, "head"),
            P(None, None, "head"),
            P(None, None, "head"),
            P("head", None),
            P("head", None),
            P("head", None),
        ),
        out_specs=(P("ctx", "head"), P("ctx", "head")),
        check_vma=False,
    )
```

```python
import functools
import math

import jax
import jax.numpy as jnp
from jax import lax
from jax.experimental import pallas as pl
from jax.experimental.pallas import tpu as pltpu

from jax.sharding import PartitionSpec as P

HD = 128


EPSILON = 1e-06


def split_heads(matrix):
    return matrix.reshape(matrix.shape[0], -1, HD).transpose(1, 0, 2)


def join_heads(blocks):
    return blocks.transpose(1, 0, 2).reshape(blocks.shape[1], -1)


def attend(queries, keys, values):
    scale = HD ** (-0.5)

    def one_head(operands):
        query_block, key_block, value_block = operands
        scores = jnp.dot(query_block, key_block.T, preferred_element_type=jnp.float32) * scale
        highest = jnp.max(scores, axis=1, keepdims=True)
        weights = jnp.exp(scores - highest)
        totals = jnp.sum(weights, axis=1, keepdims=True)
        return (
            jnp.dot(weights.astype(jnp.bfloat16), value_block, preferred_element_type=jnp.float32)
            / totals
        )

    blocks = lax.map(one_head, (split_heads(queries), split_heads(keys), split_heads(values)))
    return join_heads(blocks).astype(jnp.bfloat16)


def plain_body(
    video,
    audio,
    video_gain,
    audio_gain,
    video_qkv,
    video_cross,
    audio_cross,
    video_out,
    cross_video_out,
    cross_audio_out,
):
    scale = HD ** (-0.5)
    video_wide = video.astype(jnp.float32)
    audio_wide = audio.astype(jnp.float32)
    video_squares, audio_squares = lax.psum(
        (jnp.sum(video_wide * video_wide, axis=1), jnp.sum(audio_wide * audio_wide, axis=1)), "head"
    )
    video_rate = lax.rsqrt(video_squares / video_qkv.shape[0] + EPSILON)
    audio_rate = lax.rsqrt(audio_squares / audio_cross.shape[0] + EPSILON)
    video_scaled = (video_wide * video_gain).astype(jnp.bfloat16)
    audio_scaled = (audio_wide * audio_gain).astype(jnp.bfloat16)
    self_weight = video_qkv.reshape(video_qkv.shape[0], -1)
    mixed_weight = video_cross.reshape(video_cross.shape[0], -1)
    audio_weight = audio_cross.reshape(audio_cross.shape[0], -1)
    self_width = video_qkv.shape[2]
    cross_width = video_cross.shape[2]
    video_rows = video.shape[0]
    segment = lax.all_gather(video_scaled, "head", axis=1, tiled=True)
    self_acc = jnp.dot(segment, self_weight, preferred_element_type=jnp.float32)
    mixed_acc = jnp.dot(segment, mixed_weight, preferred_element_type=jnp.float32)
    audio_acc = jnp.dot(
        lax.all_gather(audio_scaled, "head", axis=1, tiled=True),
        audio_weight,
        preferred_element_type=jnp.float32,
    )
    self_proj = (self_acc * video_rate[:, None]).astype(jnp.bfloat16)
    video_mixed = (mixed_acc * video_rate[:, None]).astype(jnp.bfloat16)
    audio_mixed = (audio_acc * audio_rate[:, None]).astype(jnp.bfloat16)
    query_heads = split_heads(self_proj[:, :self_width])
    local_heads = query_heads.shape[0]
    running_max = jnp.full((local_heads, video_rows), -1e30, jnp.float32)
    key_heads = split_heads(
        lax.all_gather(self_proj[:, self_width : 2 * self_width], "ctx", axis=0, tiled=True)
    )
    value_heads = split_heads(
        lax.all_gather(self_proj[:, 2 * self_width :], "ctx", axis=0, tiled=True)
    )
    scores = (
        jnp.einsum("hqd,hkd->hqk", query_heads, key_heads, preferred_element_type=jnp.float32)
        * scale
    )
    newest = jnp.maximum(running_max, jnp.max(scores, axis=2))
    weights = jnp.exp(scores - newest[:, :, None])
    running_sum = jnp.sum(weights, axis=2)
    running_acc = jnp.einsum(
        "hqk,hkd->hqd",
        weights.astype(jnp.bfloat16),
        value_heads,
        preferred_element_type=jnp.float32,
    )
    self_out = join_heads(running_acc / running_sum[:, :, None]).astype(jnp.bfloat16)
    audio_key_all, audio_value_all = (
        lax.all_gather(audio_mixed[:, cross_width : 2 * cross_width], "ctx", axis=0, tiled=True),
        lax.all_gather(audio_mixed[:, 2 * cross_width :], "ctx", axis=0, tiled=True),
    )
    video_cross_out = attend(video_mixed[:, :cross_width], audio_key_all, audio_value_all)
    queries_av = audio_mixed[:, :cross_width]
    keys_av = video_mixed[:, cross_width : 2 * cross_width]
    values_av = video_mixed[:, 2 * cross_width :]
    every_query = lax.all_gather(queries_av, "ctx", axis=0, tiled=True)
    scores = (
        jnp.einsum(
            "hqd,hkd->hqk",
            split_heads(every_query),
            split_heads(keys_av),
            preferred_element_type=jnp.float32,
        )
        * scale
    )
    highest = lax.pmax(jnp.max(scores, axis=2), "ctx")
    weights = jnp.exp(scores - highest[:, :, None])
    numerators = jnp.einsum(
        "hqk,hkd->hqd",
        weights.astype(jnp.bfloat16),
        split_heads(values_av),
        preferred_element_type=jnp.float32,
    )
    weight_totals = jnp.sum(weights, axis=2)
    own_numer, own_totals = (
        lax.psum_scatter(
            numerators.astype(jnp.bfloat16), "ctx", scatter_dimension=1, tiled=True
        ).astype(jnp.float32),
        lax.psum_scatter(
            weight_totals.astype(jnp.bfloat16), "ctx", scatter_dimension=1, tiled=True
        ).astype(jnp.float32),
    )
    audio_cross_out = join_heads(own_numer / own_totals[:, :, None]).astype(jnp.bfloat16)
    video_partial = jnp.dot(self_out, video_out, preferred_element_type=jnp.float32) + jnp.dot(
        video_cross_out, cross_video_out, preferred_element_type=jnp.float32
    )
    audio_partial = jnp.dot(audio_cross_out, cross_audio_out, preferred_element_type=jnp.float32)
    video_sum, audio_sum = (
        lax.psum_scatter(
            video_partial.astype(jnp.bfloat16), "head", scatter_dimension=1, tiled=True
        ).astype(jnp.float32),
        lax.psum_scatter(
            audio_partial.astype(jnp.bfloat16), "head", scatter_dimension=1, tiled=True
        ).astype(jnp.float32),
    )
    return (
        (video_wide + video_sum).astype(jnp.bfloat16),
        (audio_wide + audio_sum).astype(jnp.bfloat16),
    )


MESH = pl.DeviceIdType.MESH
F32 = jnp.float32
BF16 = jnp.bfloat16
VMEM_LIMIT = 63 * 1024 * 1024
CHUNK = HD
SCORE_SCALE = HD ** (-0.5) * math.log2(math.e)


def head_peer(me, flip):
    low = me % 2
    mid = (me // 2) % 2
    high = me // 4
    if flip & 1:
        low = 1 - low
    if flip & 2:
        mid = 1 - mid
    if flip & 4:
        high = 1 - high
    return high * 4 + mid * 2 + low


def remote(source, target, send, recv, device):
    return pltpu.make_async_remote_copy(
        src_ref=source,
        dst_ref=target,
        send_sem=send,
        recv_sem=recv,
        device_id=device,
        device_id_type=MESH,
    )


def diagonal(rows):
    line = lax.broadcasted_iota(jnp.int32, (rows, HD), 0)
    lane = lax.broadcasted_iota(jnp.int32, (rows, HD), 1)
    return line == lane


def to_row(column):
    rows = column.shape[0]
    spread = jnp.broadcast_to(column, (rows, HD))
    return jnp.sum(jnp.where(diagonal(rows), spread, 0.0), axis=0, keepdims=True)


def to_column(row, rows):
    spread = jnp.broadcast_to(row, (rows, HD))
    return jnp.sum(jnp.where(diagonal(rows), spread, 0.0), axis=1, keepdims=True)


def contract_last(left, right):
    return lax.dot_general(left, right, (((1,), (1,)), ((), ())), preferred_element_type=F32)


def softmax_parts(query, keys, values):
    scores = [contract_last(query, key) for key in keys]
    highest = functools.reduce(
        jnp.maximum, [jnp.max(score, axis=1, keepdims=True) for score in scores]
    )
    total = 0.0
    mixed = 0.0
    for score, value in zip(scores, values):
        weight = jnp.exp2((score - highest) * SCORE_SCALE)
        total = total + jnp.sum(weight, axis=1, keepdims=True)
        mixed = mixed + jnp.dot(weight.astype(BF16), value, preferred_element_type=F32)
    return mixed, total, highest * SCORE_SCALE


def aligned(start, size):
    return pl.ds(pl.multiple_of(start, size), size)


def block_kernel(
    ctx_size,
    video_ref,
    audio_ref,
    video_gain_ref,
    audio_gain_ref,
    w_self_ref,
    w_cross_ref,
    w_audio_ref,
    w_out_ref,
    w_cross_out_ref,
    w_audio_out_ref,
    video_out_ref,
    audio_out_ref,
    xs,
    xa,
    raw,
    squares,
    every_square,
    tone_squares,
    every_tone_square,
    w_self,
    w_cross,
    w_audio,
    w_out,
    w_cross_out,
    w_audio_out,
    heads,
    sources,
    cross,
    cross_out,
    tones,
    parts,
    parts_in,
    stats,
    stats_in,
    own,
    mixed_out,
    chip,
    landed,
    tone_part,
    tone_chip,
    tone_landed,
    load,
    plane_send,
    plane_recv,
    tone_send,
    tone_recv,
    square_send,
    square_recv,
    key_send,
    key_recv,
    query_send,
    query_recv,
    back_send,
    back_recv,
    late_send,
    late_recv,
    side_send,
    side_recv,
    hop_send,
    hop_recv,
    tone_out_send,
    tone_out_recv,
):
    ctx = lax.axis_index("ctx")
    me = lax.axis_index("head")
    rows, width = video_ref.shape
    audio_rows, audio_width = audio_ref.shape
    every_tone = ctx_size * audio_rows
    count = rows // CHUNK
    local_heads = width // HD
    cross_width = w_cross.shape[2]
    cross_heads = cross_width // HD
    peer = [head_peer(me, flip) for flip in range(8)]
    mates = [(ctx + d) % ctx_size for d in range(ctx_size)]
    others = range(1, ctx_size)

    def loader(slot, source, target):
        return pltpu.make_async_copy(source, target, load.at[slot])

    loads = [
        loader(0, w_self_ref.at[1], w_self.at[1]),
        loader(1, w_self_ref.at[2], w_self.at[2]),
        loader(2, w_self_ref.at[0], w_self.at[0]),
        loader(3, w_cross_ref, w_cross),
        loader(4, w_audio_ref, w_audio),
        loader(5, w_out_ref, w_out),
        loader(6, w_cross_out_ref, w_cross_out),
        loader(7, w_audio_out_ref, w_audio_out),
    ]
    for one in loads:
        one.start()

    barrier = pltpu.get_barrier_semaphore()
    friends = [(ctx, peer[flip]) for flip in range(1, 8)]
    friends += [(mates[d], me) for d in others]
    for friend in friends:
        pl.semaphore_signal(barrier, inc=1, device_id=friend, device_id_type=MESH)

    def at_rows(k):
        return aligned(k * CHUNK, CHUNK)

    def columns(block):
        return aligned(block * width, width)

    def tone_columns(block):
        return aligned(block * audio_width, audio_width)

    my_tones = aligned(ctx * audio_rows, audio_rows)
    for k in range(count):
        wide = video_ref[pl.ds(k * CHUNK, CHUNK)].astype(F32)
        xs[pl.ds(k * CHUNK, CHUNK), columns(me)] = (wide * video_gain_ref[...]).astype(BF16)
        squares[k : k + 1] = to_row(jnp.sum(wide * wide, axis=1, keepdims=True))
    every_square[0] = squares[...]
    raw[my_tones] = audio_ref[...]

    pl.semaphore_wait(barrier, len(friends))

    def hop(slot, k):
        flip, block = (slot, me) if slot in (1, 2, 4, 6) else (1, peer[slot - 1])
        part = xs.at[at_rows(k), columns(block)]
        return remote(
            part, part, plane_send.at[slot - 1, k], plane_recv.at[slot - 1, k], (ctx, peer[flip])
        )

    def tone_hop(slot):
        flip, block = (slot, me) if slot in (1, 2, 4, 6) else (1, peer[slot - 1])
        part = xa.at[:, tone_columns(block)]
        return remote(
            part, part, tone_send.at[slot - 1], tone_recv.at[slot - 1], (ctx, peer[flip])
        )

    def square_hop(kind, flip):
        source, target = (
            (tone_squares, every_tone_square) if kind else (squares, every_square)
        )
        return remote(
            source,
            target.at[flip],
            square_send.at[kind, flip - 1],
            square_recv.at[kind, flip - 1],
            (ctx, peer[flip]),
        )

    def late_copy(kind, d):
        source, target = {
            0: (audio_ref, raw.at[my_tones]),
            1: (parts.at[mates[d]], parts_in.at[ctx]),
            2: (stats.at[mates[d]], stats_in.at[ctx]),
        }[kind]
        return remote(
            source, target, late_send.at[kind, d - 1], late_recv.at[kind, d - 1], (mates[d], me)
        )

    def key_copy(k, d):
        return remote(
            heads.at[mates[d], pl.ds(1, 2), at_rows(k)],
            sources.at[ctx, pl.ds(1, 2), at_rows(k)],
            key_send.at[d - 1, k],
            key_recv.at[d - 1, k],
            (mates[d], me),
        )

    def query_copy(k, d):
        return remote(
            heads.at[mates[d], 0, at_rows(k)],
            sources.at[ctx, 0, at_rows(k)],
            query_send.at[d - 1, k],
            query_recv.at[d - 1, k],
            (mates[d], me),
        )

    for d in others:
        late_copy(0, d).start()
    for slot in (6, 2, 4, 1):
        hop(slot, 0).start()
    for flip in range(1, 8):
        square_hop(0, flip).start()

    def begin(k, carry):
        for slot in (6, 2, 4, 1):
            hop(slot, k).start()
        return carry

    lax.fori_loop(1, count, begin, 0)

    for d in others:
        late_copy(0, d).wait_recv()
    tone_squares[...] = jnp.zeros_like(tone_squares)
    for d in range(ctx_size):
        at = pl.ds(d * audio_rows, audio_rows)
        wide = raw[at].astype(F32)
        xa[at, tone_columns(me)] = (wide * audio_gain_ref[...]).astype(BF16)
        tone_squares[d : d + 1] = to_row(jnp.sum(wide * wide, axis=1, keepdims=True))
    every_tone_square[0] = tone_squares[...]
    for one in loads[:4]:
        one.wait()
    for flip in range(1, 8):
        square_hop(0, flip).wait_recv()
    for flip in range(1, 8):
        square_hop(1, flip).start()
    for slot in (6, 2, 4, 1):
        tone_hop(slot).start()

    def video_rate(k):
        sums = jnp.sum(every_square[:, pl.ds(k, 1), :], axis=0)
        return to_column(lax.rsqrt(sums / (8 * width) + EPSILON), CHUNK)

    def cross_project(k):
        at = at_rows(k)
        rate = video_rate(k)

        def one(plane, carry):
            acc = jnp.dot(xs[at, :], w_cross[plane], preferred_element_type=F32)
            scaled = (acc * rate).astype(BF16)
            for h in range(cross_heads):
                cross[h, plane, at] = scaled[:, h * HD : (h + 1) * HD]
            return carry

        lax.fori_loop(0, 3, one, 0)

    def project(k, carry):
        at = at_rows(k)
        for slot in (2, 4, 6):
            hop(slot, k).wait_recv()
            hop(slot + 1, k).start()

        @pl.when(k > 0)
        def _():
            cross_project(k - 1)

        for slot in (1, 3, 5, 7):
            hop(slot, k).wait_recv()
        rate = video_rate(k)

        def one(i, carry):
            plane = (i + 1) % 3
            acc = jnp.dot(xs[at, :], w_self[plane], preferred_element_type=F32)
            scaled = (acc * rate).astype(BF16)
            for h in range(local_heads):
                heads[h, plane, at] = scaled[:, h * HD : (h + 1) * HD]

            @pl.when(i == 1)
            def _():
                for d in others:
                    key_copy(k, d).start()

            return carry

        lax.fori_loop(0, 3, one, 0)
        for plane in range(3):
            sources[ctx, plane, at] = heads[ctx, plane, at]
        return carry

    lax.fori_loop(0, count, project, 0)

    def ship(k, carry):
        for d in others:
            query_copy(k, d).start()
        return carry

    lax.fori_loop(0, count, ship, 0)
    cross_project(count - 1)

    for slot in (2, 4, 6):
        tone_hop(slot).wait_recv()
        tone_hop(slot + 1).start()
    loads[4].wait()
    for flip in range(1, 8):
        square_hop(1, flip).wait_recv()
    for slot in (1, 3, 5, 7):
        tone_hop(slot).wait_recv()
    tone_sums = jnp.sum(every_tone_square[...], axis=0)
    tone_rates = lax.rsqrt(tone_sums / (8 * audio_width) + EPSILON)
    rate = jnp.concatenate(
        [to_column(tone_rates[d : d + 1], audio_rows) for d in range(ctx_size)], axis=0
    )
    for plane in range(3):
        acc = jnp.dot(xa[...], w_audio[plane], preferred_element_type=F32)
        tones[:, plane * cross_width : (plane + 1) * cross_width] = (acc * rate).astype(BF16)

    sound_tile = math.gcd(rows, 256)

    def tone_part_of(plane, h):
        return slice(plane * cross_width + h * HD, plane * cross_width + (h + 1) * HD)

    for h in range(cross_heads):
        lanes = slice(h * HD, (h + 1) * HD)

        def answer(d, carry):
            query = tones[aligned(d * audio_rows, audio_rows), tone_part_of(0, h)]
            mixed, total, highest = softmax_parts(query, [cross[h, 1]], [cross[h, 2]])
            parts[d, :, lanes] = (mixed / total).astype(BF16)
            stats[d, 2 * h : 2 * h + 1] = to_row(total)
            stats[d, 2 * h + 1 : 2 * h + 2] = to_row(highest)
            return carry

        lax.fori_loop(0, ctx_size, answer, 0)
    for d in others:
        late_copy(1, d).start()
        late_copy(2, d).start()
    parts_in[ctx] = parts[ctx]
    stats_in[ctx] = stats[ctx]
    for h in range(cross_heads):
        lanes = slice(h * HD, (h + 1) * HD)

        def ask(i, carry):
            tile = aligned(i * sound_tile, sound_tile)
            mixed, total, _ = softmax_parts(
                cross[h, 0, tile], [tones[:, tone_part_of(1, h)]], [tones[:, tone_part_of(2, h)]]
            )
            cross_out[tile, lanes] = (mixed / total).astype(BF16)
            return carry

        lax.fori_loop(0, rows // sound_tile, ask, 0)

    def settle_hops(k, carry):
        for slot in range(1, 8):
            hop(slot, k).wait_send()
        for d in others:
            key_copy(k, d).wait_recv()
        return carry

    lax.fori_loop(0, count, settle_hops, 0)
    for one in loads[5:]:
        one.wait()

    def reducer(part_at, chip, landed, at, side_sems, hop_sems, out_ref, base_ref, parity):
        near_flip, end_flip = (4, 2) if parity else (2, 4)
        near, end = near_flip // 2, end_flip // 2

        def side(i):
            return remote(
                part_at(peer[2 * i + 1]), chip.at[i, at], *side_sems(i), (ctx, peer[1])
            )

        def hop(slot, flip, k):
            return remote(chip.at[k, at], landed.at[slot, at], *hop_sems(slot), (ctx, peer[flip]))

        def far_hop():
            return hop(0, near_flip, 3)

        def near_hop():
            return hop(1, near_flip, near)

        def end_hop():
            return hop(2, end_flip, end)

        def start():
            for i in (3, near, end, 0):
                side(i).start()

        def fold(i):
            side(i).wait_recv()
            chip[i, at] = (
                chip[i, at].astype(F32) + part_at(peer[2 * i])[...].astype(F32)
            ).astype(BF16)

        def join():
            fold(3)
            far_hop().start()
            fold(near)
            near_hop().start()
            fold(end)

        def pass_on():
            far_hop().wait_recv()
            chip[end, at] = (chip[end, at].astype(F32) + landed[0, at].astype(F32)).astype(BF16)
            end_hop().start()

        def close():
            side(0).wait_recv()
            total = chip[0, at].astype(F32) + part_at(me)[...].astype(F32)
            total = total + base_ref[at].astype(F32)
            near_hop().wait_recv()
            total = total + landed[1, at].astype(F32)
            end_hop().wait_recv()
            out_ref[at] = (total + landed[2, at].astype(F32)).astype(BF16)

        def settle():
            for i in range(4):
                side(i).wait_send()
            for one in (far_hop(), near_hop(), end_hop()):
                one.wait_send()

        return start, join, pass_on, close, settle

    def video_steps(k, parity):
        return reducer(
            lambda block: xs.at[at_rows(k), columns(block)],
            chip,
            landed,
            at_rows(k),
            lambda i: (side_send.at[i, k], side_recv.at[i, k]),
            lambda slot: (hop_send.at[slot, k], hop_recv.at[slot, k]),
            video_out_ref,
            video_ref,
            parity,
        )

    tone_start, tone_join, tone_pass, tone_close, tone_settle = reducer(
        lambda block: tone_part.at[block],
        tone_chip,
        tone_landed,
        pl.ds(0, audio_rows),
        lambda i: (tone_out_send.at[i], tone_out_recv.at[i]),
        lambda slot: (tone_out_send.at[4 + slot], tone_out_recv.at[4 + slot]),
        audio_out_ref,
        audio_ref,
        0,
    )

    def sound():
        for d in others:
            late_copy(1, d).wait_recv()
            late_copy(2, d).wait_recv()
        pieces = []
        for h in range(cross_heads):
            lanes = slice(h * HD, (h + 1) * HD)
            totals = [stats_in[s, 2 * h : 2 * h + 1] for s in range(ctx_size)]
            highs = [stats_in[s, 2 * h + 1 : 2 * h + 2] for s in range(ctx_size)]
            top = functools.reduce(jnp.maximum, highs)
            shares = [total * jnp.exp2(high - top) for total, high in zip(totals, highs)]
            whole = functools.reduce(jnp.add, shares)
            mixed = 0.0
            for s in range(ctx_size):
                share = to_column(shares[s] / whole, audio_rows)
                mixed = mixed + parts_in[s, :, lanes].astype(F32) * share
            pieces.append(mixed.astype(BF16))
        result = jnp.concatenate(pieces, axis=1)
        for n in range(8):
            tone_part[n] = jnp.dot(
                result,
                w_audio_out[:, n * audio_width : (n + 1) * audio_width],
                preferred_element_type=F32,
            ).astype(BF16)
        tone_start()

    def back(k, d):
        return remote(
            own.at[mates[d], at_rows(k)],
            mixed_out.at[ctx, at_rows(k)],
            back_send.at[d - 1, k],
            back_recv.at[d - 1, k],
            (mates[d], me),
        )

    def attend_pair(k, first):
        at = at_rows(k)
        pair = [mates[(first + i) % ctx_size] for i in range(2)]
        query = jnp.concatenate([sources[s, 0, at] for s in pair], axis=0)
        mixed, total, _ = softmax_parts(
            query,
            [sources[s, 1] for s in range(ctx_size)],
            [sources[s, 2] for s in range(ctx_size)],
        )
        done = (mixed / total).astype(BF16)
        for i, s in enumerate(pair):
            own[s, at] = done[i * CHUNK : (i + 1) * CHUNK]
            d = (first + i) % ctx_size
            if d:
                back(k, d).start()
            else:
                mixed_out[ctx, at] = done[i * CHUNK : (i + 1) * CHUNK]

    def output(k):
        at = at_rows(k)
        for d in others:
            back(k, d).wait_recv()
        selfs = jnp.concatenate([mixed_out[s, at] for s in range(ctx_size)], axis=1)

        def one(n, carry):
            cols = columns(n)
            xs[at, cols] = (
                jnp.dot(selfs, w_out[:, cols], preferred_element_type=F32)
                + jnp.dot(cross_out[at], w_cross_out[:, cols], preferred_element_type=F32)
            ).astype(BF16)
            return carry

        lax.fori_loop(0, 8, one, 0)
        video_steps(k, 0)[0]()

    def turn(k, parity):
        for d in others:
            query_copy(k, d).wait_recv()
        attend_pair(k, 1)

        @pl.when(k >= 2)
        def _():
            video_steps(k - 2, parity)[1]()

        attend_pair(k, 3)

        @pl.when(k >= 3)
        def _():
            video_steps(k - 3, 1 - parity)[2]()

        @pl.when(k >= 1)
        def _():
            output(k - 1)

        @pl.when(k >= 4)
        def _():
            video_steps(k - 4, parity)[3]()

    def two(i, carry):
        turn(2 * i, 0)

        @pl.when(i == 1)
        def _():
            sound()

        @pl.when(i == 2)
        def _():
            tone_pass()

        turn(2 * i + 1, 1)

        @pl.when(i == 1)
        def _():
            tone_join()

        return carry

    lax.fori_loop(0, count // 2, two, 0)
    last = count - 1
    video_steps(last - 1, 0)[1]()
    video_steps(last - 2, 1)[2]()
    output(last)
    tone_close()
    video_steps(last, 1)[1]()
    video_steps(last - 1, 0)[2]()
    video_steps(last - 3, 0)[3]()
    video_steps(last - 2, 1)[3]()
    video_steps(last, 1)[2]()
    video_steps(last - 1, 0)[3]()
    video_steps(last, 1)[3]()

    def finish(k, carry):
        for d in others:
            key_copy(k, d).wait_send()
            query_copy(k, d).wait_send()
            back(k, d).wait_send()
        video_steps(k, 0)[4]()
        return carry

    lax.fori_loop(0, count, finish, 0)
    for d in others:
        for kind in range(3):
            late_copy(kind, d).wait_send()
    for slot in range(1, 8):
        tone_hop(slot).wait_send()
    for flip in range(1, 8):
        for kind in range(2):
            square_hop(kind, flip).wait_send()
    tone_settle()


def fast_body(
    ctx_size,
    video,
    audio,
    video_gain,
    audio_gain,
    video_qkv,
    video_cross,
    audio_cross,
    video_out,
    cross_video_out,
    cross_audio_out,
):
    rows, width = video.shape
    audio_rows, audio_width = audio.shape
    depth = video_qkv.shape[0]
    audio_depth = audio_cross.shape[0]
    cross_width = video_cross.shape[2]
    count = rows // CHUNK
    cross_heads = cross_width // HD
    lines = (count + 7) // 8 * 8
    others = ctx_size - 1
    every_tone = ctx_size * audio_rows
    vmem = pl.BlockSpec(memory_space=pltpu.VMEM)
    anywhere = pl.BlockSpec(memory_space=pl.ANY)

    def wide(*shape):
        return pltpu.VMEM(shape, BF16)

    def fine(*shape):
        return pltpu.VMEM(shape, F32)

    def pair(*shape):
        return [pltpu.SemaphoreType.DMA(shape)] * 2

    return pl.pallas_call(
        functools.partial(block_kernel, ctx_size),
        out_shape=(
            jax.ShapeDtypeStruct(video.shape, BF16),
            jax.ShapeDtypeStruct(audio.shape, BF16),
        ),
        in_specs=[vmem] * 4 + [anywhere] * 6,
        out_specs=(vmem, vmem),
        scratch_shapes=[
            wide(rows, depth),
            wide(every_tone, audio_depth),
            wide(every_tone, audio_width),
            fine(lines, HD),
            fine(8, lines, HD),
            fine(8, HD),
            fine(8, 8, HD),
            wide(3, depth, width),
            wide(3, depth, cross_width),
            wide(3, audio_depth, cross_width),
            wide(*video_out.shape),
            wide(*cross_video_out.shape),
            wide(*cross_audio_out.shape),
            wide(ctx_size, 3, rows, HD),
            wide(ctx_size, 3, rows, HD),
            wide(cross_heads, 3, rows, HD),
            wide(rows, cross_width),
            wide(every_tone, 3 * cross_width),
            wide(ctx_size, audio_rows, cross_width),
            wide(ctx_size, audio_rows, cross_width),
            fine(ctx_size, 8, HD),
            fine(ctx_size, 8, HD),
            wide(ctx_size, rows, HD),
            wide(ctx_size, rows, HD),
            wide(4, rows, width),
            wide(3, rows, width),
            wide(8, audio_rows, audio_width),
            wide(4, audio_rows, audio_width),
            wide(3, audio_rows, audio_width),
            pltpu.SemaphoreType.DMA((8,)),
            *pair(7, count),
            *pair(7),
            *pair(2, 7),
            *pair(others, count),
            *pair(others, count),
            *pair(others, count),
            *pair(3, others),
            *pair(4, count),
            *pair(3, count),
            *pair(7),
        ],
        compiler_params=pltpu.CompilerParams(
            collective_id=0, has_side_effects=True, vmem_limit_bytes=VMEM_LIMIT
        ),
        name="block",
    )(
        video,
        audio,
        video_gain.reshape(1, -1),
        audio_gain.reshape(1, -1),
        video_qkv.transpose(1, 0, 2),
        video_cross.transpose(1, 0, 2),
        audio_cross.transpose(1, 0, 2),
        video_out,
        cross_video_out,
        cross_audio_out,
    )


def suits(ctx_size, head_size, video, audio, video_cross):
    rows, width = video.shape
    audio_rows, audio_width = audio.shape
    return (
        head_size == 8
        and ctx_size == 4
        and width == ctx_size * HD
        and rows % (2 * CHUNK) == 0
        and rows >= 6 * CHUNK
        and audio_rows % 16 == 0
        and audio_rows <= HD
        and audio_width % HD == 0
        and video_cross.shape[2] % HD == 0
        and video_cross.shape[2] <= 4 * HD
    )


def solution(mesh):
    ctx_size = mesh.shape["ctx"]

    def body(*operands):
        if suits(ctx_size, mesh.shape["head"], operands[0], operands[1], operands[5]):
            return fast_body(ctx_size, *operands)
        return plain_body(*operands)

    return jax.shard_map(
        body,
        mesh=mesh,
        in_specs=(
            P("ctx", "head"),
            P("ctx", "head"),
            P("head"),
            P("head"),
            P(None, None, "head"),
            P(None, None, "head"),
            P(None, None, "head"),
            P("head", None),
            P("head", None),
            P("head", None),
        ),
        out_specs=(P("ctx", "head"), P("ctx", "head")),
        check_vma=False,
    )
```

```python
import functools
import math

import jax
import jax.numpy as jnp
from jax import lax
from jax.experimental import pallas as pl
from jax.experimental.pallas import tpu as pltpu

from jax.sharding import PartitionSpec as P

HD = 128


EPSILON = 1e-06


def split_heads(matrix):
    return matrix.reshape(matrix.shape[0], -1, HD).transpose(1, 0, 2)


def join_heads(blocks):
    return blocks.transpose(1, 0, 2).reshape(blocks.shape[1], -1)


def attend(queries, keys, values):
    scale = HD ** (-0.5)

    def one_head(operands):
        query_block, key_block, value_block = operands
        scores = jnp.dot(query_block, key_block.T, preferred_element_type=jnp.float32) * scale
        highest = jnp.max(scores, axis=1, keepdims=True)
        weights = jnp.exp(scores - highest)
        totals = jnp.sum(weights, axis=1, keepdims=True)
        return (
            jnp.dot(weights.astype(jnp.bfloat16), value_block, preferred_element_type=jnp.float32)
            / totals
        )

    blocks = lax.map(one_head, (split_heads(queries), split_heads(keys), split_heads(values)))
    return join_heads(blocks).astype(jnp.bfloat16)


def plain_body(
    video,
    audio,
    video_gain,
    audio_gain,
    video_qkv,
    video_cross,
    audio_cross,
    video_out,
    cross_video_out,
    cross_audio_out,
):
    scale = HD ** (-0.5)
    video_wide = video.astype(jnp.float32)
    audio_wide = audio.astype(jnp.float32)
    video_squares, audio_squares = lax.psum(
        (jnp.sum(video_wide * video_wide, axis=1), jnp.sum(audio_wide * audio_wide, axis=1)), "head"
    )
    video_rate = lax.rsqrt(video_squares / video_qkv.shape[0] + EPSILON)
    audio_rate = lax.rsqrt(audio_squares / audio_cross.shape[0] + EPSILON)
    video_scaled = (video_wide * video_gain).astype(jnp.bfloat16)
    audio_scaled = (audio_wide * audio_gain).astype(jnp.bfloat16)
    self_weight = video_qkv.reshape(video_qkv.shape[0], -1)
    mixed_weight = video_cross.reshape(video_cross.shape[0], -1)
    audio_weight = audio_cross.reshape(audio_cross.shape[0], -1)
    self_width = video_qkv.shape[2]
    cross_width = video_cross.shape[2]
    video_rows = video.shape[0]
    segment = lax.all_gather(video_scaled, "head", axis=1, tiled=True)
    self_acc = jnp.dot(segment, self_weight, preferred_element_type=jnp.float32)
    mixed_acc = jnp.dot(segment, mixed_weight, preferred_element_type=jnp.float32)
    audio_acc = jnp.dot(
        lax.all_gather(audio_scaled, "head", axis=1, tiled=True),
        audio_weight,
        preferred_element_type=jnp.float32,
    )
    self_proj = (self_acc * video_rate[:, None]).astype(jnp.bfloat16)
    video_mixed = (mixed_acc * video_rate[:, None]).astype(jnp.bfloat16)
    audio_mixed = (audio_acc * audio_rate[:, None]).astype(jnp.bfloat16)
    query_heads = split_heads(self_proj[:, :self_width])
    local_heads = query_heads.shape[0]
    running_max = jnp.full((local_heads, video_rows), -1e30, jnp.float32)
    key_heads = split_heads(
        lax.all_gather(self_proj[:, self_width : 2 * self_width], "ctx", axis=0, tiled=True)
    )
    value_heads = split_heads(
        lax.all_gather(self_proj[:, 2 * self_width :], "ctx", axis=0, tiled=True)
    )
    scores = (
        jnp.einsum("hqd,hkd->hqk", query_heads, key_heads, preferred_element_type=jnp.float32)
        * scale
    )
    newest = jnp.maximum(running_max, jnp.max(scores, axis=2))
    weights = jnp.exp(scores - newest[:, :, None])
    running_sum = jnp.sum(weights, axis=2)
    running_acc = jnp.einsum(
        "hqk,hkd->hqd",
        weights.astype(jnp.bfloat16),
        value_heads,
        preferred_element_type=jnp.float32,
    )
    self_out = join_heads(running_acc / running_sum[:, :, None]).astype(jnp.bfloat16)
    audio_key_all, audio_value_all = (
        lax.all_gather(audio_mixed[:, cross_width : 2 * cross_width], "ctx", axis=0, tiled=True),
        lax.all_gather(audio_mixed[:, 2 * cross_width :], "ctx", axis=0, tiled=True),
    )
    video_cross_out = attend(video_mixed[:, :cross_width], audio_key_all, audio_value_all)
    queries_av = audio_mixed[:, :cross_width]
    keys_av = video_mixed[:, cross_width : 2 * cross_width]
    values_av = video_mixed[:, 2 * cross_width :]
    every_query = lax.all_gather(queries_av, "ctx", axis=0, tiled=True)
    scores = (
        jnp.einsum(
            "hqd,hkd->hqk",
            split_heads(every_query),
            split_heads(keys_av),
            preferred_element_type=jnp.float32,
        )
        * scale
    )
    highest = lax.pmax(jnp.max(scores, axis=2), "ctx")
    weights = jnp.exp(scores - highest[:, :, None])
    numerators = jnp.einsum(
        "hqk,hkd->hqd",
        weights.astype(jnp.bfloat16),
        split_heads(values_av),
        preferred_element_type=jnp.float32,
    )
    weight_totals = jnp.sum(weights, axis=2)
    own_numer, own_totals = (
        lax.psum_scatter(
            numerators.astype(jnp.bfloat16), "ctx", scatter_dimension=1, tiled=True
        ).astype(jnp.float32),
        lax.psum_scatter(
            weight_totals.astype(jnp.bfloat16), "ctx", scatter_dimension=1, tiled=True
        ).astype(jnp.float32),
    )
    audio_cross_out = join_heads(own_numer / own_totals[:, :, None]).astype(jnp.bfloat16)
    video_partial = jnp.dot(self_out, video_out, preferred_element_type=jnp.float32) + jnp.dot(
        video_cross_out, cross_video_out, preferred_element_type=jnp.float32
    )
    audio_partial = jnp.dot(audio_cross_out, cross_audio_out, preferred_element_type=jnp.float32)
    video_sum, audio_sum = (
        lax.psum_scatter(
            video_partial.astype(jnp.bfloat16), "head", scatter_dimension=1, tiled=True
        ).astype(jnp.float32),
        lax.psum_scatter(
            audio_partial.astype(jnp.bfloat16), "head", scatter_dimension=1, tiled=True
        ).astype(jnp.float32),
    )
    return (
        (video_wide + video_sum).astype(jnp.bfloat16),
        (audio_wide + audio_sum).astype(jnp.bfloat16),
    )


MESH = pl.DeviceIdType.MESH
F32 = jnp.float32
BF16 = jnp.bfloat16
VMEM_LIMIT = 63 * 1024 * 1024
CHUNK = HD
SCORE_SCALE = HD ** (-0.5) * math.log2(math.e)


def head_peer(me, flip):
    low = me % 2
    mid = (me // 2) % 2
    high = me // 4
    if flip & 1:
        low = 1 - low
    if flip & 2:
        mid = 1 - mid
    if flip & 4:
        high = 1 - high
    return high * 4 + mid * 2 + low


def remote(source, target, send, recv, device):
    return pltpu.make_async_remote_copy(
        src_ref=source,
        dst_ref=target,
        send_sem=send,
        recv_sem=recv,
        device_id=device,
        device_id_type=MESH,
    )


def diagonal(rows):
    line = lax.broadcasted_iota(jnp.int32, (rows, HD), 0)
    lane = lax.broadcasted_iota(jnp.int32, (rows, HD), 1)
    return line == lane


def to_row(column):
    rows = column.shape[0]
    spread = jnp.broadcast_to(column, (rows, HD))
    return jnp.sum(jnp.where(diagonal(rows), spread, 0.0), axis=0, keepdims=True)


def to_column(row, rows):
    spread = jnp.broadcast_to(row, (rows, HD))
    return jnp.sum(jnp.where(diagonal(rows), spread, 0.0), axis=1, keepdims=True)


def contract_last(left, right):
    return lax.dot_general(left, right, (((1,), (1,)), ((), ())), preferred_element_type=F32)


def softmax_parts(query, keys, values):
    scores = [contract_last(query, key) for key in keys]
    highest = functools.reduce(
        jnp.maximum, [jnp.max(score, axis=1, keepdims=True) for score in scores]
    )
    total = 0.0
    mixed = 0.0
    for score, value in zip(scores, values):
        weight = jnp.exp2((score - highest) * SCORE_SCALE)
        total = total + jnp.sum(weight, axis=1, keepdims=True)
        mixed = mixed + jnp.dot(weight.astype(BF16), value, preferred_element_type=F32)
    return mixed, total, highest * SCORE_SCALE


def aligned(start, size):
    return pl.ds(pl.multiple_of(start, size), size)


def block_kernel(
    ctx_size,
    video_ref,
    audio_ref,
    video_gain_ref,
    audio_gain_ref,
    w_self_ref,
    w_cross_ref,
    w_audio_ref,
    w_out_ref,
    w_cross_out_ref,
    w_audio_out_ref,
    video_out_ref,
    audio_out_ref,
    xs,
    xa,
    raw,
    squares,
    every_square,
    tone_squares,
    every_tone_square,
    w_self,
    w_cross,
    w_audio,
    w_out,
    w_cross_out,
    w_audio_out,
    heads,
    sources,
    cross,
    tones,
    parts,
    parts_in,
    stats,
    stats_in,
    own,
    mixed_out,
    chip,
    landed,
    tone_part,
    tone_chip,
    tone_landed,
    load,
    plane_send,
    plane_recv,
    tone_send,
    tone_recv,
    square_send,
    square_recv,
    key_send,
    key_recv,
    query_send,
    query_recv,
    back_send,
    back_recv,
    late_send,
    late_recv,
    side_send,
    side_recv,
    hop_send,
    hop_recv,
    tone_out_send,
    tone_out_recv,
):
    ctx = lax.axis_index("ctx")
    me = lax.axis_index("head")
    rows, width = video_ref.shape
    audio_rows, audio_width = audio_ref.shape
    count = rows // CHUNK
    local_heads = width // HD
    cross_width = w_cross.shape[2]
    cross_heads = cross_width // HD
    peer = [head_peer(me, flip) for flip in range(8)]
    mates = [(ctx + d) % ctx_size for d in range(ctx_size)]
    others = range(1, ctx_size)

    def loader(slot, source, target):
        return pltpu.make_async_copy(source, target, load.at[slot])

    loads = [
        loader(0, w_self_ref.at[1], w_self.at[1]),
        loader(1, w_self_ref.at[2], w_self.at[2]),
        loader(2, w_self_ref.at[0], w_self.at[0]),
        loader(3, w_cross_ref, w_cross),
        loader(4, w_audio_ref, w_audio),
        loader(5, w_out_ref, w_out),
        loader(6, w_cross_out_ref, w_cross_out),
        loader(7, w_audio_out_ref, w_audio_out),
    ]
    for one in loads:
        one.start()

    barrier = pltpu.get_barrier_semaphore()
    friends = [(ctx, peer[flip]) for flip in range(1, 8)]
    friends += [(mates[d], me) for d in others]
    for friend in friends:
        pl.semaphore_signal(barrier, inc=1, device_id=friend, device_id_type=MESH)

    def at_rows(k):
        return aligned(k * CHUNK, CHUNK)

    def columns(block):
        return aligned(block * width, width)

    def tone_columns(block):
        return aligned(block * audio_width, audio_width)

    my_tones = aligned(ctx * audio_rows, audio_rows)

    def scale(k):
        wide = video_ref[pl.ds(k * CHUNK, CHUNK)].astype(F32)
        xs[pl.ds(k * CHUNK, CHUNK), columns(me)] = (wide * video_gain_ref[...]).astype(BF16)
        squares[k : k + 1] = to_row(jnp.sum(wide * wide, axis=1, keepdims=True))

    scale(0)
    raw[my_tones] = audio_ref[...]
    pl.semaphore_wait(barrier, len(friends))

    def hop(slot, k):
        flip, block = (slot, me) if slot in (1, 2, 4, 6) else (1, peer[slot - 1])
        part = xs.at[at_rows(k), columns(block)]
        return remote(
            part, part, plane_send.at[slot - 1, k], plane_recv.at[slot - 1, k], (ctx, peer[flip])
        )

    def tone_hop(slot):
        flip, block = (slot, me) if slot in (1, 2, 4, 6) else (1, peer[slot - 1])
        part = xa.at[:, tone_columns(block)]
        return remote(
            part, part, tone_send.at[slot - 1], tone_recv.at[slot - 1], (ctx, peer[flip])
        )

    def square_hop(kind, flip):
        source, target = (
            (tone_squares, every_tone_square) if kind else (squares, every_square)
        )
        return remote(
            source,
            target.at[flip],
            square_send.at[kind, flip - 1],
            square_recv.at[kind, flip - 1],
            (ctx, peer[flip]),
        )

    def late_copy(kind, d):
        source, target = {
            0: (audio_ref, raw.at[my_tones]),
            1: (parts.at[mates[d]], parts_in.at[ctx]),
            2: (stats.at[mates[d]], stats_in.at[ctx]),
        }[kind]
        return remote(
            source, target, late_send.at[kind, d - 1], late_recv.at[kind, d - 1], (mates[d], me)
        )

    def key_copy(k, d):
        return remote(
            heads.at[mates[d], pl.ds(1, 2), at_rows(k)],
            sources.at[ctx, pl.ds(1, 2), at_rows(k)],
            key_send.at[d - 1, k],
            key_recv.at[d - 1, k],
            (mates[d], me),
        )

    def query_copy(k, d):
        return remote(
            heads.at[mates[d], 0, at_rows(k)],
            sources.at[ctx, 0, at_rows(k)],
            query_send.at[d - 1, k],
            query_recv.at[d - 1, k],
            (mates[d], me),
        )

    for slot in (6, 2, 4, 1):
        hop(slot, 0).start()
    for d in others:
        late_copy(0, d).start()
    for k in range(1, count):
        scale(k)
    every_square[0] = squares[...]
    for flip in range(1, 8):
        square_hop(0, flip).start()

    def begin(k, carry):
        for slot in (6, 2, 4, 1):
            hop(slot, k).start()
        return carry

    lax.fori_loop(1, count, begin, 0)

    for d in others:
        late_copy(0, d).wait_recv()
    tone_squares[...] = jnp.zeros_like(tone_squares)
    for d in range(ctx_size):
        at = pl.ds(d * audio_rows, audio_rows)
        wide = raw[at].astype(F32)
        xa[at, tone_columns(me)] = (wide * audio_gain_ref[...]).astype(BF16)
        tone_squares[d : d + 1] = to_row(jnp.sum(wide * wide, axis=1, keepdims=True))
    every_tone_square[0] = tone_squares[...]
    for one in loads[:4]:
        one.wait()
    for flip in range(1, 8):
        square_hop(0, flip).wait_recv()
    for flip in range(1, 8):
        square_hop(1, flip).start()
    for slot in (6, 2, 4, 1):
        tone_hop(slot).start()

    def video_rate(k):
        sums = jnp.sum(every_square[:, pl.ds(k, 1), :], axis=0)
        return to_column(lax.rsqrt(sums / (8 * width) + EPSILON), CHUNK)

    def cross_project(k):
        at = at_rows(k)
        rate = video_rate(k)

        def one(plane, carry):
            acc = jnp.dot(xs[at, :], w_cross[plane], preferred_element_type=F32)
            scaled = (acc * rate).astype(BF16)
            for h in range(cross_heads):
                cross[h, plane, at] = scaled[:, h * HD : (h + 1) * HD]
            return carry

        lax.fori_loop(0, 3, one, 0)

    def ship(k):
        for d in others:
            query_copy(k, d).start()

    def project(k, carry):
        at = at_rows(k)
        for slot in (2, 4, 6):
            hop(slot, k).wait_recv()
            hop(slot + 1, k).start()

        @pl.when(k > 0)
        def _():
            cross_project(k - 1)

        for slot in (1, 3, 5, 7):
            hop(slot, k).wait_recv()
        rate = video_rate(k)

        def one(i, carry):
            plane = (i + 1) % 3
            acc = jnp.dot(xs[at, :], w_self[plane], preferred_element_type=F32)
            scaled = (acc * rate).astype(BF16)
            for h in range(local_heads):
                heads[h, plane, at] = scaled[:, h * HD : (h + 1) * HD]

            @pl.when(i == 1)
            def _():
                for d in others:
                    key_copy(k, d).start()

            return carry

        lax.fori_loop(0, 3, one, 0)

        @pl.when(k == count - 2)
        def _():
            ship(0)

        for plane in range(3):
            sources[ctx, plane, at] = heads[ctx, plane, at]
        return carry

    lax.fori_loop(0, count, project, 0)

    ship(1)
    ship(2)
    cross_project(count - 1)


    def tone_project():
        for slot in (2, 4, 6):
            tone_hop(slot).wait_recv()
            tone_hop(slot + 1).start()
        loads[4].wait()
        for flip in range(1, 8):
            square_hop(1, flip).wait_recv()
        for slot in (1, 3, 5, 7):
            tone_hop(slot).wait_recv()
        tone_sums = jnp.sum(every_tone_square[...], axis=0)
        tone_rates = lax.rsqrt(tone_sums / (8 * audio_width) + EPSILON)
        rate = jnp.concatenate(
            [to_column(tone_rates[d : d + 1], audio_rows) for d in range(ctx_size)], axis=0
        )
        for plane in range(3):
            acc = jnp.dot(xa[...], w_audio[plane], preferred_element_type=F32)
            tones[:, plane * cross_width : (plane + 1) * cross_width] = (acc * rate).astype(BF16)

    def tone_part_of(plane, h):
        return slice(plane * cross_width + h * HD, plane * cross_width + (h + 1) * HD)

    def answer():
        for h in range(cross_heads):
            lanes = slice(h * HD, (h + 1) * HD)

            def one(d, carry):
                query = tones[aligned(d * audio_rows, audio_rows), tone_part_of(0, h)]
                mixed, total, highest = softmax_parts(query, [cross[h, 1]], [cross[h, 2]])
                parts[d, :, lanes] = (mixed / total).astype(BF16)
                stats[d, 2 * h : 2 * h + 1] = to_row(total)
                stats[d, 2 * h + 1 : 2 * h + 2] = to_row(highest)
                return carry

            lax.fori_loop(0, ctx_size, one, 0)
        for d in others:
            late_copy(1, d).start()
            late_copy(2, d).start()
        parts_in[ctx] = parts[ctx]
        stats_in[ctx] = stats[ctx]

    def ask(k):
        at = at_rows(k)
        pieces = []
        for h in range(cross_heads):
            mixed, total, _ = softmax_parts(
                cross[h, 0, at], [tones[:, tone_part_of(1, h)]], [tones[:, tone_part_of(2, h)]]
            )
            pieces.append((mixed / total).astype(BF16))
        return jnp.concatenate(pieces, axis=1)

    def settle_hops(k, carry):
        for slot in range(1, 8):
            hop(slot, k).wait_send()
        for d in others:
            key_copy(k, d).wait_recv()
        return carry

    lax.fori_loop(0, count, settle_hops, 0)
    for one in loads[5:]:
        one.wait()
    ones = jnp.ones((rows, HD), BF16)
    for s in range(ctx_size):
        w_self[0, s * rows : (s + 1) * rows, :HD] = sources[s, 2]
        w_self[0, s * rows : (s + 1) * rows, HD : 2 * HD] = ones

    def reducer(part_at, chip, landed, at, side_sems, hop_sems, out_ref, base_ref):
        def side(i):
            return remote(
                part_at(peer[2 * i + 1]), chip.at[i, at], *side_sems(i), (ctx, peer[1])
            )

        def hop(i):
            return remote(
                chip.at[i, at], landed.at[i - 1, at], *hop_sems(i - 1), (ctx, peer[2 * i])
            )

        def start():
            for i in (3, 1, 2, 0):
                side(i).start()

        def join():
            for i in (3, 1, 2):
                side(i).wait_recv()
                chip[i, at] = (
                    chip[i, at].astype(F32) + part_at(peer[2 * i])[...].astype(F32)
                ).astype(BF16)
                hop(i).start()

        def close():
            side(0).wait_recv()
            total = chip[0, at].astype(F32) + part_at(me)[...].astype(F32)
            total = total + base_ref[at].astype(F32)
            for i in (1, 2, 3):
                hop(i).wait_recv()
                total = total + landed[i - 1, at].astype(F32)
            out_ref[at] = total.astype(BF16)

        def settle():
            for i in range(4):
                side(i).wait_send()
            for i in (1, 2, 3):
                hop(i).wait_send()

        return start, join, close, settle

    def video_steps(k):
        return reducer(
            lambda block: xs.at[at_rows(k), columns(block)],
            chip,
            landed,
            at_rows(k),
            lambda i: (side_send.at[i, k], side_recv.at[i, k]),
            lambda slot: (hop_send.at[slot, k], hop_recv.at[slot, k]),
            video_out_ref,
            video_ref,
        )

    tone_start, tone_join, tone_close, tone_settle = reducer(
        lambda block: tone_part.at[block],
        tone_chip,
        tone_landed,
        pl.ds(0, audio_rows),
        lambda i: (tone_out_send.at[i], tone_out_recv.at[i]),
        lambda slot: (tone_out_send.at[4 + slot], tone_out_recv.at[4 + slot]),
        audio_out_ref,
        audio_ref,
    )

    def sound():
        for d in others:
            late_copy(1, d).wait_recv()
            late_copy(2, d).wait_recv()
        pieces = []
        for h in range(cross_heads):
            lanes = slice(h * HD, (h + 1) * HD)
            totals = [stats_in[s, 2 * h : 2 * h + 1] for s in range(ctx_size)]
            highs = [stats_in[s, 2 * h + 1 : 2 * h + 2] for s in range(ctx_size)]
            top = functools.reduce(jnp.maximum, highs)
            shares = [total * jnp.exp2(high - top) for total, high in zip(totals, highs)]
            whole = functools.reduce(jnp.add, shares)
            mixed = 0.0
            for s in range(ctx_size):
                share = to_column(shares[s] / whole, audio_rows)
                mixed = mixed + parts_in[s, :, lanes].astype(F32) * share
            pieces.append(mixed.astype(BF16))
        result = jnp.concatenate(pieces, axis=1)
        for n in range(8):
            tone_part[n] = jnp.dot(
                result,
                w_audio_out[:, n * audio_width : (n + 1) * audio_width],
                preferred_element_type=F32,
            ).astype(BF16)
        tone_start()

    def back(k, d):
        return remote(
            own.at[mates[d], at_rows(k)],
            mixed_out.at[ctx, at_rows(k)],
            back_send.at[d - 1, k],
            back_recv.at[d - 1, k],
            (mates[d], me),
        )

    def attend_pair(k, first):
        at = at_rows(k)
        pair = [mates[(first + i) % ctx_size] for i in range(2)]
        query = jnp.concatenate([sources[s, 0, at] for s in pair], axis=0)
        scores = [contract_last(query, sources[s, 1]) for s in range(ctx_size)]
        highest = jnp.max(scores[0], axis=1, keepdims=True)
        mixed = None
        for s in range(ctx_size):
            if s:
                higher = jnp.maximum(highest, jnp.max(scores[s], axis=1, keepdims=True))
                fade = jnp.exp2((highest - higher) * SCORE_SCALE)
                highest = higher
            weight = jnp.exp2((scores[s] - highest) * SCORE_SCALE).astype(BF16)
            step = jnp.dot(
                weight,
                w_self[0, s * rows : (s + 1) * rows, : 2 * HD],
                preferred_element_type=F32,
            )
            mixed = mixed * fade + step if s else step
        done = (mixed[:, :HD] / mixed[:, HD:]).astype(BF16)
        for i, s in enumerate(pair):
            own[s, at] = done[i * CHUNK : (i + 1) * CHUNK]
            d = (first + i) % ctx_size
            if d:
                back(k, d).start()
            else:
                mixed_out[ctx, at] = done[i * CHUNK : (i + 1) * CHUNK]

    def output(k):
        at = at_rows(k)
        for d in others:
            back(k, d).wait_recv()
        selfs = jnp.concatenate([mixed_out[s, at] for s in range(ctx_size)], axis=1)
        crossed = ask(k)

        def one(n, carry):
            cols = columns(n)
            xs[at, cols] = (
                jnp.dot(selfs, w_out[:, cols], preferred_element_type=F32)
                + jnp.dot(crossed, w_cross_out[:, cols], preferred_element_type=F32)
            ).astype(BF16)
            return carry

        lax.fori_loop(0, 8, one, 0)
        video_steps(k)[0]()

    def turn(k, carry):
        for d in others:
            query_copy(k, d).wait_recv()
        attend_pair(k, 1)

        @pl.when(k >= 3)
        def _():
            video_steps(k - 3)[1]()

        attend_pair(k, 3)

        @pl.when(k + 3 < count)
        def _():
            ship(k + 3)

        @pl.when(k >= 2)
        def _():
            output(k - 2)

        @pl.when(k >= 5)
        def _():
            video_steps(k - 5)[2]()

        for step, work in ((0, tone_project), (1, answer), (3, sound), (4, tone_join)):
            pl.when(k == step)(work)
        return carry

    lax.fori_loop(0, count, turn, 0)
    last = count - 1
    video_steps(last - 2)[1]()
    output(last - 1)
    tone_close()
    video_steps(last - 4)[2]()
    video_steps(last - 1)[1]()
    output(last)
    video_steps(last - 3)[2]()
    video_steps(last)[1]()
    video_steps(last - 2)[2]()
    video_steps(last - 1)[2]()
    video_steps(last)[2]()

    def finish(k, carry):
        for d in others:
            key_copy(k, d).wait_send()
            query_copy(k, d).wait_send()
            back(k, d).wait_send()
        video_steps(k)[3]()
        return carry

    lax.fori_loop(0, count, finish, 0)
    for d in others:
        for kind in range(3):
            late_copy(kind, d).wait_send()
    for slot in range(1, 8):
        tone_hop(slot).wait_send()
    for flip in range(1, 8):
        for kind in range(2):
            square_hop(kind, flip).wait_send()
    tone_settle()


def fast_body(
    ctx_size,
    video,
    audio,
    video_gain,
    audio_gain,
    video_qkv,
    video_cross,
    audio_cross,
    video_out,
    cross_video_out,
    cross_audio_out,
):
    rows, width = video.shape
    audio_rows, audio_width = audio.shape
    depth = video_qkv.shape[0]
    audio_depth = audio_cross.shape[0]
    cross_width = video_cross.shape[2]
    count = rows // CHUNK
    cross_heads = cross_width // HD
    lines = (count + 7) // 8 * 8
    others = ctx_size - 1
    every_tone = ctx_size * audio_rows
    vmem = pl.BlockSpec(memory_space=pltpu.VMEM)
    anywhere = pl.BlockSpec(memory_space=pl.ANY)

    def wide(*shape):
        return pltpu.VMEM(shape, BF16)

    def fine(*shape):
        return pltpu.VMEM(shape, F32)

    def pair(*shape):
        return [pltpu.SemaphoreType.DMA(shape)] * 2

    return pl.pallas_call(
        functools.partial(block_kernel, ctx_size),
        out_shape=(
            jax.ShapeDtypeStruct(video.shape, BF16),
            jax.ShapeDtypeStruct(audio.shape, BF16),
        ),
        in_specs=[vmem] * 4 + [anywhere] * 6,
        out_specs=(vmem, vmem),
        scratch_shapes=[
            wide(rows, depth),
            wide(every_tone, audio_depth),
            wide(every_tone, audio_width),
            fine(lines, HD),
            fine(8, lines, HD),
            fine(8, HD),
            fine(8, 8, HD),
            wide(3, depth, width),
            wide(3, depth, cross_width),
            wide(3, audio_depth, cross_width),
            wide(*video_out.shape),
            wide(*cross_video_out.shape),
            wide(*cross_audio_out.shape),
            wide(ctx_size, 3, rows, HD),
            wide(ctx_size, 3, rows, HD),
            wide(cross_heads, 3, rows, HD),
            wide(every_tone, 3 * cross_width),
            wide(ctx_size, audio_rows, cross_width),
            wide(ctx_size, audio_rows, cross_width),
            fine(ctx_size, 8, HD),
            fine(ctx_size, 8, HD),
            wide(ctx_size, rows, HD),
            wide(ctx_size, rows, HD),
            wide(4, rows, width),
            wide(3, rows, width),
            wide(8, audio_rows, audio_width),
            wide(4, audio_rows, audio_width),
            wide(3, audio_rows, audio_width),
            pltpu.SemaphoreType.DMA((8,)),
            *pair(7, count),
            *pair(7),
            *pair(2, 7),
            *pair(others, count),
            *pair(others, count),
            *pair(others, count),
            *pair(3, others),
            *pair(4, count),
            *pair(3, count),
            *pair(7),
        ],
        compiler_params=pltpu.CompilerParams(
            collective_id=0, has_side_effects=True, vmem_limit_bytes=VMEM_LIMIT
        ),
        name="block",
    )(
        video,
        audio,
        video_gain.reshape(1, -1),
        audio_gain.reshape(1, -1),
        video_qkv.transpose(1, 0, 2),
        video_cross.transpose(1, 0, 2),
        audio_cross.transpose(1, 0, 2),
        video_out,
        cross_video_out,
        cross_audio_out,
    )


def suits(ctx_size, head_size, video, audio, video_cross):
    rows, width = video.shape
    audio_rows, audio_width = audio.shape
    return (
        head_size == 8
        and ctx_size == 4
        and width == ctx_size * HD
        and rows % CHUNK == 0
        and rows >= 6 * CHUNK
        and audio_rows % 16 == 0
        and audio_rows <= HD
        and audio_width % HD == 0
        and video_cross.shape[2] % HD == 0
        and video_cross.shape[2] <= 4 * HD
        and ctx_size * rows <= video_cross.shape[0]
    )


def solution(mesh):
    ctx_size = mesh.shape["ctx"]

    def body(*operands):
        if suits(ctx_size, mesh.shape["head"], operands[0], operands[1], operands[5]):
            return fast_body(ctx_size, *operands)
        return plain_body(*operands)

    return jax.shard_map(
        body,
        mesh=mesh,
        in_specs=(
            P("ctx", "head"),
            P("ctx", "head"),
            P("head"),
            P("head"),
            P(None, None, "head"),
            P(None, None, "head"),
            P(None, None, "head"),
            P("head", None),
            P("head", None),
            P("head", None),
        ),
        out_specs=(P("ctx", "head"), P("ctx", "head")),
        check_vma=False,
    )
```

```python
import functools
import math

import jax
import jax.numpy as jnp
from jax import lax
from jax.experimental import pallas as pl
from jax.experimental.pallas import tpu as pltpu

from jax.sharding import PartitionSpec as P

HD = 128


EPSILON = 1e-06


def split_heads(matrix):
    return matrix.reshape(matrix.shape[0], -1, HD).transpose(1, 0, 2)


def join_heads(blocks):
    return blocks.transpose(1, 0, 2).reshape(blocks.shape[1], -1)


def attend(queries, keys, values):
    scale = HD ** (-0.5)

    def one_head(operands):
        query_block, key_block, value_block = operands
        scores = jnp.dot(query_block, key_block.T, preferred_element_type=jnp.float32) * scale
        highest = jnp.max(scores, axis=1, keepdims=True)
        weights = jnp.exp(scores - highest)
        totals = jnp.sum(weights, axis=1, keepdims=True)
        return (
            jnp.dot(weights.astype(jnp.bfloat16), value_block, preferred_element_type=jnp.float32)
            / totals
        )

    blocks = lax.map(one_head, (split_heads(queries), split_heads(keys), split_heads(values)))
    return join_heads(blocks).astype(jnp.bfloat16)


def plain_body(
    video,
    audio,
    video_gain,
    audio_gain,
    video_qkv,
    video_cross,
    audio_cross,
    video_out,
    cross_video_out,
    cross_audio_out,
):
    scale = HD ** (-0.5)
    video_wide = video.astype(jnp.float32)
    audio_wide = audio.astype(jnp.float32)
    video_squares, audio_squares = lax.psum(
        (jnp.sum(video_wide * video_wide, axis=1), jnp.sum(audio_wide * audio_wide, axis=1)), "head"
    )
    video_rate = lax.rsqrt(video_squares / video_qkv.shape[0] + EPSILON)
    audio_rate = lax.rsqrt(audio_squares / audio_cross.shape[0] + EPSILON)
    video_scaled = (video_wide * video_gain).astype(jnp.bfloat16)
    audio_scaled = (audio_wide * audio_gain).astype(jnp.bfloat16)
    self_weight = video_qkv.reshape(video_qkv.shape[0], -1)
    mixed_weight = video_cross.reshape(video_cross.shape[0], -1)
    audio_weight = audio_cross.reshape(audio_cross.shape[0], -1)
    self_width = video_qkv.shape[2]
    cross_width = video_cross.shape[2]
    video_rows = video.shape[0]
    segment = lax.all_gather(video_scaled, "head", axis=1, tiled=True)
    self_acc = jnp.dot(segment, self_weight, preferred_element_type=jnp.float32)
    mixed_acc = jnp.dot(segment, mixed_weight, preferred_element_type=jnp.float32)
    audio_acc = jnp.dot(
        lax.all_gather(audio_scaled, "head", axis=1, tiled=True),
        audio_weight,
        preferred_element_type=jnp.float32,
    )
    self_proj = (self_acc * video_rate[:, None]).astype(jnp.bfloat16)
    video_mixed = (mixed_acc * video_rate[:, None]).astype(jnp.bfloat16)
    audio_mixed = (audio_acc * audio_rate[:, None]).astype(jnp.bfloat16)
    query_heads = split_heads(self_proj[:, :self_width])
    local_heads = query_heads.shape[0]
    running_max = jnp.full((local_heads, video_rows), -1e30, jnp.float32)
    key_heads = split_heads(
        lax.all_gather(self_proj[:, self_width : 2 * self_width], "ctx", axis=0, tiled=True)
    )
    value_heads = split_heads(
        lax.all_gather(self_proj[:, 2 * self_width :], "ctx", axis=0, tiled=True)
    )
    scores = (
        jnp.einsum("hqd,hkd->hqk", query_heads, key_heads, preferred_element_type=jnp.float32)
        * scale
    )
    newest = jnp.maximum(running_max, jnp.max(scores, axis=2))
    weights = jnp.exp(scores - newest[:, :, None])
    running_sum = jnp.sum(weights, axis=2)
    running_acc = jnp.einsum(
        "hqk,hkd->hqd",
        weights.astype(jnp.bfloat16),
        value_heads,
        preferred_element_type=jnp.float32,
    )
    self_out = join_heads(running_acc / running_sum[:, :, None]).astype(jnp.bfloat16)
    audio_key_all, audio_value_all = (
        lax.all_gather(audio_mixed[:, cross_width : 2 * cross_width], "ctx", axis=0, tiled=True),
        lax.all_gather(audio_mixed[:, 2 * cross_width :], "ctx", axis=0, tiled=True),
    )
    video_cross_out = attend(video_mixed[:, :cross_width], audio_key_all, audio_value_all)
    queries_av = audio_mixed[:, :cross_width]
    keys_av = video_mixed[:, cross_width : 2 * cross_width]
    values_av = video_mixed[:, 2 * cross_width :]
    every_query = lax.all_gather(queries_av, "ctx", axis=0, tiled=True)
    scores = (
        jnp.einsum(
            "hqd,hkd->hqk",
            split_heads(every_query),
            split_heads(keys_av),
            preferred_element_type=jnp.float32,
        )
        * scale
    )
    highest = lax.pmax(jnp.max(scores, axis=2), "ctx")
    weights = jnp.exp(scores - highest[:, :, None])
    numerators = jnp.einsum(
        "hqk,hkd->hqd",
        weights.astype(jnp.bfloat16),
        split_heads(values_av),
        preferred_element_type=jnp.float32,
    )
    weight_totals = jnp.sum(weights, axis=2)
    own_numer, own_totals = (
        lax.psum_scatter(
            numerators.astype(jnp.bfloat16), "ctx", scatter_dimension=1, tiled=True
        ).astype(jnp.float32),
        lax.psum_scatter(
            weight_totals.astype(jnp.bfloat16), "ctx", scatter_dimension=1, tiled=True
        ).astype(jnp.float32),
    )
    audio_cross_out = join_heads(own_numer / own_totals[:, :, None]).astype(jnp.bfloat16)
    video_partial = jnp.dot(self_out, video_out, preferred_element_type=jnp.float32) + jnp.dot(
        video_cross_out, cross_video_out, preferred_element_type=jnp.float32
    )
    audio_partial = jnp.dot(audio_cross_out, cross_audio_out, preferred_element_type=jnp.float32)
    video_sum, audio_sum = (
        lax.psum_scatter(
            video_partial.astype(jnp.bfloat16), "head", scatter_dimension=1, tiled=True
        ).astype(jnp.float32),
        lax.psum_scatter(
            audio_partial.astype(jnp.bfloat16), "head", scatter_dimension=1, tiled=True
        ).astype(jnp.float32),
    )
    return (
        (video_wide + video_sum).astype(jnp.bfloat16),
        (audio_wide + audio_sum).astype(jnp.bfloat16),
    )


MESH = pl.DeviceIdType.MESH
F32 = jnp.float32
BF16 = jnp.bfloat16
VMEM_LIMIT = 63 * 1024 * 1024
CHUNK = HD
SCORE_SCALE = HD ** (-0.5) * math.log2(math.e)


def head_peer(me, flip):
    low = me % 2
    mid = (me // 2) % 2
    high = me // 4
    if flip & 1:
        low = 1 - low
    if flip & 2:
        mid = 1 - mid
    if flip & 4:
        high = 1 - high
    return high * 4 + mid * 2 + low


def remote(source, target, send, recv, device):
    return pltpu.make_async_remote_copy(
        src_ref=source,
        dst_ref=target,
        send_sem=send,
        recv_sem=recv,
        device_id=device,
        device_id_type=MESH,
    )


def diagonal(rows):
    line = lax.broadcasted_iota(jnp.int32, (rows, HD), 0)
    lane = lax.broadcasted_iota(jnp.int32, (rows, HD), 1)
    return line == lane


def to_row(column):
    rows = column.shape[0]
    spread = jnp.broadcast_to(column, (rows, HD))
    return jnp.sum(jnp.where(diagonal(rows), spread, 0.0), axis=0, keepdims=True)


def to_column(row, rows):
    spread = jnp.broadcast_to(row, (rows, HD))
    return jnp.sum(jnp.where(diagonal(rows), spread, 0.0), axis=1, keepdims=True)


def contract_last(left, right):
    return lax.dot_general(left, right, (((1,), (1,)), ((), ())), preferred_element_type=F32)


def softmax_parts(query, keys, values):
    scores = [contract_last(query, key) for key in keys]
    highest = functools.reduce(
        jnp.maximum, [jnp.max(score, axis=1, keepdims=True) for score in scores]
    )
    total = 0.0
    mixed = 0.0
    for score, value in zip(scores, values):
        weight = jnp.exp2((score - highest) * SCORE_SCALE)
        total = total + jnp.sum(weight, axis=1, keepdims=True)
        mixed = mixed + jnp.dot(weight.astype(BF16), value, preferred_element_type=F32)
    return mixed, total, highest * SCORE_SCALE


def aligned(start, size):
    return pl.ds(pl.multiple_of(start, size), size)


def block_kernel(
    ctx_size,
    video_ref,
    audio_ref,
    video_gain_ref,
    audio_gain_ref,
    w_self_ref,
    w_cross_ref,
    w_audio_ref,
    w_out_ref,
    w_cross_out_ref,
    w_audio_out_ref,
    video_out_ref,
    audio_out_ref,
    xs,
    xa,
    raw,
    squares,
    every_square,
    tone_squares,
    every_tone_square,
    w_self,
    w_cross,
    w_audio,
    w_out,
    w_cross_out,
    w_audio_out,
    heads,
    sources,
    cross,
    tones,
    parts,
    parts_in,
    stats,
    stats_in,
    own,
    mixed_out,
    chip,
    landed,
    tone_part,
    tone_chip,
    tone_landed,
    load,
    plane_send,
    plane_recv,
    tone_send,
    tone_recv,
    square_send,
    square_recv,
    key_send,
    key_recv,
    query_send,
    query_recv,
    back_send,
    back_recv,
    late_send,
    late_recv,
    side_send,
    side_recv,
    hop_send,
    hop_recv,
    tone_out_send,
    tone_out_recv,
):
    ctx = lax.axis_index("ctx")
    me = lax.axis_index("head")
    rows, width = video_ref.shape
    audio_rows, audio_width = audio_ref.shape
    count = rows // CHUNK
    local_heads = width // HD
    cross_width = w_cross.shape[2]
    cross_heads = cross_width // HD
    peer = [head_peer(me, flip) for flip in range(8)]
    mates = [(ctx + d) % ctx_size for d in range(ctx_size)]
    others = range(1, ctx_size)

    def loader(slot, source, target):
        return pltpu.make_async_copy(source, target, load.at[slot])

    loads = [
        loader(0, w_self_ref.at[1], w_self.at[1]),
        loader(1, w_self_ref.at[2], w_self.at[2]),
        loader(2, w_self_ref.at[0], w_self.at[0]),
        loader(3, w_cross_ref, w_cross),
        loader(4, w_audio_ref, w_audio),
        loader(5, w_out_ref, w_out),
        loader(6, w_cross_out_ref, w_cross_out),
        loader(7, w_audio_out_ref, w_audio_out),
    ]
    for one in loads:
        one.start()

    barrier = pltpu.get_barrier_semaphore()
    friends = [(ctx, peer[flip]) for flip in range(1, 8)]
    friends += [(mates[d], me) for d in others]
    for friend in friends:
        pl.semaphore_signal(barrier, inc=1, device_id=friend, device_id_type=MESH)

    def at_rows(k):
        return aligned(k * CHUNK, CHUNK)

    def columns(block):
        return aligned(block * width, width)

    def tone_columns(block):
        return aligned(block * audio_width, audio_width)

    my_tones = aligned(ctx * audio_rows, audio_rows)

    def scale(k):
        wide = video_ref[pl.ds(k * CHUNK, CHUNK)].astype(F32)
        xs[pl.ds(k * CHUNK, CHUNK), columns(me)] = (wide * video_gain_ref[...]).astype(BF16)
        squares[k : k + 1] = to_row(jnp.sum(wide * wide, axis=1, keepdims=True))

    scale(0)
    raw[my_tones] = audio_ref[...]
    pl.semaphore_wait(barrier, len(friends))

    def hop(slot, k):
        flip, block = (slot, me) if slot in (1, 2, 4, 6) else (1, peer[slot - 1])
        part = xs.at[at_rows(k), columns(block)]
        return remote(
            part, part, plane_send.at[slot - 1, k], plane_recv.at[slot - 1, k], (ctx, peer[flip])
        )

    def tone_hop(slot):
        flip, block = (slot, me) if slot in (1, 2, 4, 6) else (1, peer[slot - 1])
        part = xa.at[:, tone_columns(block)]
        return remote(
            part, part, tone_send.at[slot - 1], tone_recv.at[slot - 1], (ctx, peer[flip])
        )

    def square_hop(kind, flip):
        source, target = (
            (tone_squares, every_tone_square) if kind else (squares, every_square)
        )
        return remote(
            source,
            target.at[flip],
            square_send.at[kind, flip - 1],
            square_recv.at[kind, flip - 1],
            (ctx, peer[flip]),
        )

    def late_copy(kind, d):
        source, target = {
            0: (audio_ref, raw.at[my_tones]),
            1: (parts.at[mates[d]], parts_in.at[ctx]),
            2: (stats.at[mates[d]], stats_in.at[ctx]),
        }[kind]
        return remote(
            source, target, late_send.at[kind, d - 1], late_recv.at[kind, d - 1], (mates[d], me)
        )

    def key_copy(k, d):
        return remote(
            heads.at[mates[d], pl.ds(1, 2), at_rows(k)],
            sources.at[ctx, pl.ds(1, 2), at_rows(k)],
            key_send.at[d - 1, k],
            key_recv.at[d - 1, k],
            (mates[d], me),
        )

    def query_copy(k, d):
        return remote(
            heads.at[mates[d], 0, at_rows(k)],
            sources.at[ctx, 0, at_rows(k)],
            query_send.at[d - 1, k],
            query_recv.at[d - 1, k],
            (mates[d], me),
        )

    for slot in (6, 2, 4, 1):
        hop(slot, 0).start()
    for d in others:
        late_copy(0, d).start()
    for k in range(1, count):
        scale(k)
    every_square[0] = squares[...]
    for flip in range(1, 8):
        square_hop(0, flip).start()

    def begin(k, carry):
        for slot in (6, 2, 4, 1):
            hop(slot, k).start()
        return carry

    lax.fori_loop(1, count, begin, 0)

    for d in others:
        late_copy(0, d).wait_recv()
    tone_squares[...] = jnp.zeros_like(tone_squares)
    for d in range(ctx_size):
        at = pl.ds(d * audio_rows, audio_rows)
        wide = raw[at].astype(F32)
        xa[at, tone_columns(me)] = (wide * audio_gain_ref[...]).astype(BF16)
        tone_squares[d : d + 1] = to_row(jnp.sum(wide * wide, axis=1, keepdims=True))
    every_tone_square[0] = tone_squares[...]
    for one in loads[:4]:
        one.wait()
    for flip in range(1, 8):
        square_hop(0, flip).wait_recv()
    for flip in range(1, 8):
        square_hop(1, flip).start()
    for slot in (6, 2, 4, 1):
        tone_hop(slot).start()

    def video_rate(k):
        sums = jnp.sum(every_square[:, pl.ds(k, 1), :], axis=0)
        return to_column(lax.rsqrt(sums / (8 * width) + EPSILON), CHUNK)

    def cross_project(k):
        at = at_rows(k)
        rate = video_rate(k)

        def one(plane, carry):
            acc = jnp.dot(xs[at, :], w_cross[plane], preferred_element_type=F32)
            scaled = (acc * rate).astype(BF16)
            for h in range(cross_heads):
                cross[h, plane, at] = scaled[:, h * HD : (h + 1) * HD]
            return carry

        lax.fori_loop(0, 3, one, 0)

    def ship(k):
        for d in others:
            query_copy(k, d).start()

    def project(k, carry):
        at = at_rows(k)
        for slot in (2, 4, 6):
            hop(slot, k).wait_recv()
            hop(slot + 1, k).start()

        @pl.when(k > 0)
        def _():
            cross_project(k - 1)

        for slot in (1, 3, 5, 7):
            hop(slot, k).wait_recv()
        rate = video_rate(k)

        def one(i, carry):
            plane = (i + 1) % 3
            acc = jnp.dot(xs[at, :], w_self[plane], preferred_element_type=F32)
            scaled = (acc * rate).astype(BF16)
            for h in range(local_heads):
                heads[h, plane, at] = scaled[:, h * HD : (h + 1) * HD]

            @pl.when(i == 1)
            def _():
                for d in others:
                    key_copy(k, d).start()

            return carry

        lax.fori_loop(0, 3, one, 0)

        @pl.when(k == count - 2)
        def _():
            ship(0)

        for plane in range(3):
            sources[ctx, plane, at] = heads[ctx, plane, at]
        return carry

    lax.fori_loop(0, count, project, 0)

    ship(1)
    cross_project(count - 1)


    def tone_project():
        for slot in (2, 4, 6):
            tone_hop(slot).wait_recv()
            tone_hop(slot + 1).start()
        loads[4].wait()
        for flip in range(1, 8):
            square_hop(1, flip).wait_recv()
        for slot in (1, 3, 5, 7):
            tone_hop(slot).wait_recv()
        tone_sums = jnp.sum(every_tone_square[...], axis=0)
        tone_rates = lax.rsqrt(tone_sums / (8 * audio_width) + EPSILON)
        rate = jnp.concatenate(
            [to_column(tone_rates[d : d + 1], audio_rows) for d in range(ctx_size)], axis=0
        )
        for plane in range(3):
            acc = jnp.dot(xa[...], w_audio[plane], preferred_element_type=F32)
            tones[:, plane * cross_width : (plane + 1) * cross_width] = (acc * rate).astype(BF16)

    def tone_part_of(plane, h):
        return slice(plane * cross_width + h * HD, plane * cross_width + (h + 1) * HD)

    def answer():
        for h in range(cross_heads):
            lanes = slice(h * HD, (h + 1) * HD)

            def one(d, carry):
                query = tones[aligned(d * audio_rows, audio_rows), tone_part_of(0, h)]
                mixed, total, highest = softmax_parts(query, [cross[h, 1]], [cross[h, 2]])
                parts[d, :, lanes] = (mixed / total).astype(BF16)
                stats[d, 2 * h : 2 * h + 1] = to_row(total)
                stats[d, 2 * h + 1 : 2 * h + 2] = to_row(highest)
                return carry

            lax.fori_loop(0, ctx_size, one, 0)
        for d in others:
            late_copy(1, d).start()
            late_copy(2, d).start()
        parts_in[ctx] = parts[ctx]
        stats_in[ctx] = stats[ctx]

    def ask(k):
        at = at_rows(k)
        pieces = []
        for h in range(cross_heads):
            mixed, total, _ = softmax_parts(
                cross[h, 0, at], [tones[:, tone_part_of(1, h)]], [tones[:, tone_part_of(2, h)]]
            )
            pieces.append((mixed / total).astype(BF16))
        return jnp.concatenate(pieces, axis=1)

    def settle_hops(k, carry):
        for slot in range(1, 8):
            hop(slot, k).wait_send()
        for d in others:
            key_copy(k, d).wait_recv()
        return carry

    lax.fori_loop(0, count, settle_hops, 0)
    for one in loads[5:]:
        one.wait()
    ones = jnp.ones((rows, HD), BF16)
    for s in range(ctx_size):
        w_self[0, s * rows : (s + 1) * rows, :HD] = sources[s, 2]
        w_self[0, s * rows : (s + 1) * rows, HD : 2 * HD] = ones

    def reducer(part_at, chip, landed, at, side_sems, hop_sems, out_ref, base_ref):
        def side(i):
            return remote(
                part_at(peer[2 * i + 1]), chip.at[i, at], *side_sems(i), (ctx, peer[1])
            )

        def hop(i):
            return remote(
                chip.at[i, at], landed.at[i - 1, at], *hop_sems(i - 1), (ctx, peer[2 * i])
            )

        def start():
            for i in (3, 1, 2, 0):
                side(i).start()

        def join():
            for i in (3, 1, 2):
                side(i).wait_recv()
                chip[i, at] = (
                    chip[i, at].astype(F32) + part_at(peer[2 * i])[...].astype(F32)
                ).astype(BF16)
                hop(i).start()

        def close():
            side(0).wait_recv()
            total = chip[0, at].astype(F32) + part_at(me)[...].astype(F32)
            total = total + base_ref[at].astype(F32)
            for i in (1, 2, 3):
                hop(i).wait_recv()
                total = total + landed[i - 1, at].astype(F32)
            out_ref[at] = total.astype(BF16)

        def settle():
            for i in range(4):
                side(i).wait_send()
            for i in (1, 2, 3):
                hop(i).wait_send()

        return start, join, close, settle

    def video_steps(k):
        return reducer(
            lambda block: xs.at[at_rows(k), columns(block)],
            chip,
            landed,
            at_rows(k),
            lambda i: (side_send.at[i, k], side_recv.at[i, k]),
            lambda slot: (hop_send.at[slot, k], hop_recv.at[slot, k]),
            video_out_ref,
            video_ref,
        )

    tone_start, tone_join, tone_close, tone_settle = reducer(
        lambda block: tone_part.at[block],
        tone_chip,
        tone_landed,
        pl.ds(0, audio_rows),
        lambda i: (tone_out_send.at[i], tone_out_recv.at[i]),
        lambda slot: (tone_out_send.at[4 + slot], tone_out_recv.at[4 + slot]),
        audio_out_ref,
        audio_ref,
    )

    def sound():
        for d in others:
            late_copy(1, d).wait_recv()
            late_copy(2, d).wait_recv()
        pieces = []
        for h in range(cross_heads):
            lanes = slice(h * HD, (h + 1) * HD)
            totals = [stats_in[s, 2 * h : 2 * h + 1] for s in range(ctx_size)]
            highs = [stats_in[s, 2 * h + 1 : 2 * h + 2] for s in range(ctx_size)]
            top = functools.reduce(jnp.maximum, highs)
            shares = [total * jnp.exp2(high - top) for total, high in zip(totals, highs)]
            whole = functools.reduce(jnp.add, shares)
            mixed = 0.0
            for s in range(ctx_size):
                share = to_column(shares[s] / whole, audio_rows)
                mixed = mixed + parts_in[s, :, lanes].astype(F32) * share
            pieces.append(mixed.astype(BF16))
        result = jnp.concatenate(pieces, axis=1)
        for n in range(8):
            tone_part[n] = jnp.dot(
                result,
                w_audio_out[:, n * audio_width : (n + 1) * audio_width],
                preferred_element_type=F32,
            ).astype(BF16)
        tone_start()

    def back(k, d):
        return remote(
            own.at[mates[d], at_rows(k)],
            mixed_out.at[ctx, at_rows(k)],
            back_send.at[d - 1, k],
            back_recv.at[d - 1, k],
            (mates[d], me),
        )

    def attend_pair(k, first):
        at = at_rows(k)
        pair = [mates[(first + i) % ctx_size] for i in range(2)]
        query = jnp.concatenate([sources[s, 0, at] for s in pair], axis=0)
        scores = [contract_last(query, sources[s, 1]) for s in range(ctx_size)]
        highest = jnp.max(scores[0], axis=1, keepdims=True)
        mixed = None
        for s in range(ctx_size):
            if s:
                higher = jnp.maximum(highest, jnp.max(scores[s], axis=1, keepdims=True))
                fade = jnp.exp2((highest - higher) * SCORE_SCALE)
                highest = higher
            weight = jnp.exp2((scores[s] - highest) * SCORE_SCALE).astype(BF16)
            step = jnp.dot(
                weight,
                w_self[0, s * rows : (s + 1) * rows, : 2 * HD],
                preferred_element_type=F32,
            )
            mixed = mixed * fade + step if s else step
        done = (mixed[:, :HD] / mixed[:, HD:]).astype(BF16)
        for i, s in enumerate(pair):
            own[s, at] = done[i * CHUNK : (i + 1) * CHUNK]
            d = (first + i) % ctx_size
            if d:
                back(k, d).start()
            else:
                mixed_out[ctx, at] = done[i * CHUNK : (i + 1) * CHUNK]

    def output(k):
        at = at_rows(k)
        for d in others:
            back(k, d).wait_recv()
        selfs = jnp.concatenate([mixed_out[s, at] for s in range(ctx_size)], axis=1)
        crossed = ask(k)

        def one(n, carry):
            cols = columns(n)
            xs[at, cols] = (
                jnp.dot(selfs, w_out[:, cols], preferred_element_type=F32)
                + jnp.dot(crossed, w_cross_out[:, cols], preferred_element_type=F32)
            ).astype(BF16)
            return carry

        lax.fori_loop(0, 8, one, 0, unroll=2)
        video_steps(k)[0]()

    def turn(k, carry):
        for d in others:
            query_copy(k, d).wait_recv()
        attend_pair(k, 1)

        @pl.when(k >= 2)
        def _():
            video_steps(k - 2)[1]()

        attend_pair(k, 3)

        @pl.when(k + 2 < count)
        def _():
            ship(k + 2)

        @pl.when(k >= 1)
        def _():
            output(k - 1)

        @pl.when(k >= 4)
        def _():
            video_steps(k - 4)[2]()

        for step, work in ((0, tone_project), (3, answer), (4, sound), (5, tone_join)):
            pl.when(k == step)(work)
        return carry

    lax.fori_loop(0, count, turn, 0)
    last = count - 1
    video_steps(last - 1)[1]()
    video_steps(last - 3)[2]()
    output(last)
    tone_close()
    video_steps(last - 2)[2]()
    video_steps(last)[1]()
    video_steps(last - 1)[2]()
    video_steps(last)[2]()

    def finish(k, carry):
        for d in others:
            key_copy(k, d).wait_send()
            query_copy(k, d).wait_send()
            back(k, d).wait_send()
        video_steps(k)[3]()
        return carry

    lax.fori_loop(0, count, finish, 0)
    for d in others:
        for kind in range(3):
            late_copy(kind, d).wait_send()
    for slot in range(1, 8):
        tone_hop(slot).wait_send()
    for flip in range(1, 8):
        for kind in range(2):
            square_hop(kind, flip).wait_send()
    tone_settle()


def fast_body(
    ctx_size,
    video,
    audio,
    video_gain,
    audio_gain,
    video_qkv,
    video_cross,
    audio_cross,
    video_out,
    cross_video_out,
    cross_audio_out,
):
    rows, width = video.shape
    audio_rows, audio_width = audio.shape
    depth = video_qkv.shape[0]
    audio_depth = audio_cross.shape[0]
    cross_width = video_cross.shape[2]
    count = rows // CHUNK
    cross_heads = cross_width // HD
    lines = (count + 7) // 8 * 8
    others = ctx_size - 1
    every_tone = ctx_size * audio_rows
    vmem = pl.BlockSpec(memory_space=pltpu.VMEM)
    anywhere = pl.BlockSpec(memory_space=pl.ANY)

    def wide(*shape):
        return pltpu.VMEM(shape, BF16)

    def fine(*shape):
        return pltpu.VMEM(shape, F32)

    def pair(*shape):
        return [pltpu.SemaphoreType.DMA(shape)] * 2

    return pl.pallas_call(
        functools.partial(block_kernel, ctx_size),
        out_shape=(
            jax.ShapeDtypeStruct(video.shape, BF16),
            jax.ShapeDtypeStruct(audio.shape, BF16),
        ),
        in_specs=[vmem] * 4 + [anywhere] * 6,
        out_specs=(vmem, vmem),
        scratch_shapes=[
            wide(rows, depth),
            wide(every_tone, audio_depth),
            wide(every_tone, audio_width),
            fine(lines, HD),
            fine(8, lines, HD),
            fine(8, HD),
            fine(8, 8, HD),
            wide(3, depth, width),
            wide(3, depth, cross_width),
            wide(3, audio_depth, cross_width),
            wide(*video_out.shape),
            wide(*cross_video_out.shape),
            wide(*cross_audio_out.shape),
            wide(ctx_size, 3, rows, HD),
            wide(ctx_size, 3, rows, HD),
            wide(cross_heads, 3, rows, HD),
            wide(every_tone, 3 * cross_width),
            wide(ctx_size, audio_rows, cross_width),
            wide(ctx_size, audio_rows, cross_width),
            fine(ctx_size, 8, HD),
            fine(ctx_size, 8, HD),
            wide(ctx_size, rows, HD),
            wide(ctx_size, rows, HD),
            wide(4, rows, width),
            wide(3, rows, width),
            wide(8, audio_rows, audio_width),
            wide(4, audio_rows, audio_width),
            wide(3, audio_rows, audio_width),
            pltpu.SemaphoreType.DMA((8,)),
            *pair(7, count),
            *pair(7),
            *pair(2, 7),
            *pair(others, count),
            *pair(others, count),
            *pair(others, count),
            *pair(3, others),
            *pair(4, count),
            *pair(3, count),
            *pair(7),
        ],
        compiler_params=pltpu.CompilerParams(
            collective_id=0, has_side_effects=True, vmem_limit_bytes=VMEM_LIMIT
        ),
        name="block",
    )(
        video,
        audio,
        video_gain.reshape(1, -1),
        audio_gain.reshape(1, -1),
        video_qkv.transpose(1, 0, 2),
        video_cross.transpose(1, 0, 2),
        audio_cross.transpose(1, 0, 2),
        video_out,
        cross_video_out,
        cross_audio_out,
    )


def suits(ctx_size, head_size, video, audio, video_cross):
    rows, width = video.shape
    audio_rows, audio_width = audio.shape
    return (
        head_size == 8
        and ctx_size == 4
        and width == ctx_size * HD
        and rows % CHUNK == 0
        and rows >= 6 * CHUNK
        and audio_rows % 16 == 0
        and audio_rows <= HD
        and audio_width % HD == 0
        and video_cross.shape[2] % HD == 0
        and video_cross.shape[2] <= 4 * HD
        and ctx_size * rows <= video_cross.shape[0]
    )


def solution(mesh):
    ctx_size = mesh.shape["ctx"]

    def body(*operands):
        if suits(ctx_size, mesh.shape["head"], operands[0], operands[1], operands[5]):
            return fast_body(ctx_size, *operands)
        return plain_body(*operands)

    return jax.shard_map(
        body,
        mesh=mesh,
        in_specs=(
            P("ctx", "head"),
            P("ctx", "head"),
            P("head"),
            P("head"),
            P(None, None, "head"),
            P(None, None, "head"),
            P(None, None, "head"),
            P("head", None),
            P("head", None),
            P("head", None),
        ),
        out_specs=(P("ctx", "head"), P("ctx", "head")),
        check_vma=False,
    )
```

```python
import functools
import math

import jax
import jax.numpy as jnp
from jax import lax
from jax.experimental import pallas as pl
from jax.experimental.pallas import tpu as pltpu

from jax.sharding import PartitionSpec as P

HD = 128


EPSILON = 1e-06


def split_heads(matrix):
    return matrix.reshape(matrix.shape[0], -1, HD).transpose(1, 0, 2)


def join_heads(blocks):
    return blocks.transpose(1, 0, 2).reshape(blocks.shape[1], -1)


def attend(queries, keys, values):
    scale = HD ** (-0.5)

    def one_head(operands):
        query_block, key_block, value_block = operands
        scores = jnp.dot(query_block, key_block.T, preferred_element_type=jnp.float32) * scale
        highest = jnp.max(scores, axis=1, keepdims=True)
        weights = jnp.exp(scores - highest)
        totals = jnp.sum(weights, axis=1, keepdims=True)
        return (
            jnp.dot(weights.astype(jnp.bfloat16), value_block, preferred_element_type=jnp.float32)
            / totals
        )

    blocks = lax.map(one_head, (split_heads(queries), split_heads(keys), split_heads(values)))
    return join_heads(blocks).astype(jnp.bfloat16)


def plain_body(
    video,
    audio,
    video_gain,
    audio_gain,
    video_qkv,
    video_cross,
    audio_cross,
    video_out,
    cross_video_out,
    cross_audio_out,
):
    scale = HD ** (-0.5)
    video_wide = video.astype(jnp.float32)
    audio_wide = audio.astype(jnp.float32)
    video_squares, audio_squares = lax.psum(
        (jnp.sum(video_wide * video_wide, axis=1), jnp.sum(audio_wide * audio_wide, axis=1)), "head"
    )
    video_rate = lax.rsqrt(video_squares / video_qkv.shape[0] + EPSILON)
    audio_rate = lax.rsqrt(audio_squares / audio_cross.shape[0] + EPSILON)
    video_scaled = (video_wide * video_gain).astype(jnp.bfloat16)
    audio_scaled = (audio_wide * audio_gain).astype(jnp.bfloat16)
    self_weight = video_qkv.reshape(video_qkv.shape[0], -1)
    mixed_weight = video_cross.reshape(video_cross.shape[0], -1)
    audio_weight = audio_cross.reshape(audio_cross.shape[0], -1)
    self_width = video_qkv.shape[2]
    cross_width = video_cross.shape[2]
    video_rows = video.shape[0]
    segment = lax.all_gather(video_scaled, "head", axis=1, tiled=True)
    self_acc = jnp.dot(segment, self_weight, preferred_element_type=jnp.float32)
    mixed_acc = jnp.dot(segment, mixed_weight, preferred_element_type=jnp.float32)
    audio_acc = jnp.dot(
        lax.all_gather(audio_scaled, "head", axis=1, tiled=True),
        audio_weight,
        preferred_element_type=jnp.float32,
    )
    self_proj = (self_acc * video_rate[:, None]).astype(jnp.bfloat16)
    video_mixed = (mixed_acc * video_rate[:, None]).astype(jnp.bfloat16)
    audio_mixed = (audio_acc * audio_rate[:, None]).astype(jnp.bfloat16)
    query_heads = split_heads(self_proj[:, :self_width])
    local_heads = query_heads.shape[0]
    running_max = jnp.full((local_heads, video_rows), -1e30, jnp.float32)
    key_heads = split_heads(
        lax.all_gather(self_proj[:, self_width : 2 * self_width], "ctx", axis=0, tiled=True)
    )
    value_heads = split_heads(
        lax.all_gather(self_proj[:, 2 * self_width :], "ctx", axis=0, tiled=True)
    )
    scores = (
        jnp.einsum("hqd,hkd->hqk", query_heads, key_heads, preferred_element_type=jnp.float32)
        * scale
    )
    newest = jnp.maximum(running_max, jnp.max(scores, axis=2))
    weights = jnp.exp(scores - newest[:, :, None])
    running_sum = jnp.sum(weights, axis=2)
    running_acc = jnp.einsum(
        "hqk,hkd->hqd",
        weights.astype(jnp.bfloat16),
        value_heads,
        preferred_element_type=jnp.float32,
    )
    self_out = join_heads(running_acc / running_sum[:, :, None]).astype(jnp.bfloat16)
    audio_key_all, audio_value_all = (
        lax.all_gather(audio_mixed[:, cross_width : 2 * cross_width], "ctx", axis=0, tiled=True),
        lax.all_gather(audio_mixed[:, 2 * cross_width :], "ctx", axis=0, tiled=True),
    )
    video_cross_out = attend(video_mixed[:, :cross_width], audio_key_all, audio_value_all)
    queries_av = audio_mixed[:, :cross_width]
    keys_av = video_mixed[:, cross_width : 2 * cross_width]
    values_av = video_mixed[:, 2 * cross_width :]
    every_query = lax.all_gather(queries_av, "ctx", axis=0, tiled=True)
    scores = (
        jnp.einsum(
            "hqd,hkd->hqk",
            split_heads(every_query),
            split_heads(keys_av),
            preferred_element_type=jnp.float32,
        )
        * scale
    )
    highest = lax.pmax(jnp.max(scores, axis=2), "ctx")
    weights = jnp.exp(scores - highest[:, :, None])
    numerators = jnp.einsum(
        "hqk,hkd->hqd",
        weights.astype(jnp.bfloat16),
        split_heads(values_av),
        preferred_element_type=jnp.float32,
    )
    weight_totals = jnp.sum(weights, axis=2)
    own_numer, own_totals = (
        lax.psum_scatter(
            numerators.astype(jnp.bfloat16), "ctx", scatter_dimension=1, tiled=True
        ).astype(jnp.float32),
        lax.psum_scatter(
            weight_totals.astype(jnp.bfloat16), "ctx", scatter_dimension=1, tiled=True
        ).astype(jnp.float32),
    )
    audio_cross_out = join_heads(own_numer / own_totals[:, :, None]).astype(jnp.bfloat16)
    video_partial = jnp.dot(self_out, video_out, preferred_element_type=jnp.float32) + jnp.dot(
        video_cross_out, cross_video_out, preferred_element_type=jnp.float32
    )
    audio_partial = jnp.dot(audio_cross_out, cross_audio_out, preferred_element_type=jnp.float32)
    video_sum, audio_sum = (
        lax.psum_scatter(
            video_partial.astype(jnp.bfloat16), "head", scatter_dimension=1, tiled=True
        ).astype(jnp.float32),
        lax.psum_scatter(
            audio_partial.astype(jnp.bfloat16), "head", scatter_dimension=1, tiled=True
        ).astype(jnp.float32),
    )
    return (
        (video_wide + video_sum).astype(jnp.bfloat16),
        (audio_wide + audio_sum).astype(jnp.bfloat16),
    )


MESH = pl.DeviceIdType.MESH
F32 = jnp.float32
BF16 = jnp.bfloat16
VMEM_LIMIT = 63 * 1024 * 1024
CHUNK = HD
SCORE_SCALE = HD ** (-0.5) * math.log2(math.e)


def head_peer(me, flip):
    low = me % 2
    mid = (me // 2) % 2
    high = me // 4
    if flip & 1:
        low = 1 - low
    if flip & 2:
        mid = 1 - mid
    if flip & 4:
        high = 1 - high
    return high * 4 + mid * 2 + low


def remote(source, target, send, recv, device):
    return pltpu.make_async_remote_copy(
        src_ref=source,
        dst_ref=target,
        send_sem=send,
        recv_sem=recv,
        device_id=device,
        device_id_type=MESH,
    )


def diagonal(rows):
    line = lax.broadcasted_iota(jnp.int32, (rows, HD), 0)
    lane = lax.broadcasted_iota(jnp.int32, (rows, HD), 1)
    return line == lane


def to_row(column):
    rows = column.shape[0]
    spread = jnp.broadcast_to(column, (rows, HD))
    return jnp.sum(jnp.where(diagonal(rows), spread, 0.0), axis=0, keepdims=True)


def to_column(row, rows):
    spread = jnp.broadcast_to(row, (rows, HD))
    return jnp.sum(jnp.where(diagonal(rows), spread, 0.0), axis=1, keepdims=True)


def contract_last(left, right):
    return lax.dot_general(left, right, (((1,), (1,)), ((), ())), preferred_element_type=F32)


def softmax_parts(query, keys, values):
    scores = [contract_last(query, key) for key in keys]
    highest = functools.reduce(
        jnp.maximum, [jnp.max(score, axis=1, keepdims=True) for score in scores]
    )
    total = 0.0
    mixed = 0.0
    for score, value in zip(scores, values):
        weight = jnp.exp2((score - highest) * SCORE_SCALE)
        total = total + jnp.sum(weight, axis=1, keepdims=True)
        mixed = mixed + jnp.dot(weight.astype(BF16), value, preferred_element_type=F32)
    return mixed, total, highest * SCORE_SCALE


def aligned(start, size):
    return pl.ds(pl.multiple_of(start, size), size)


def block_kernel(
    ctx_size,
    video_ref,
    audio_ref,
    video_gain_ref,
    audio_gain_ref,
    w_self_ref,
    w_cross_ref,
    w_audio_ref,
    w_out_ref,
    w_cross_out_ref,
    w_audio_out_ref,
    video_out_ref,
    audio_out_ref,
    xs,
    xa,
    raw,
    squares,
    every_square,
    tone_squares,
    every_tone_square,
    w_self,
    w_cross,
    w_audio,
    w_out,
    w_cross_out,
    w_audio_out,
    heads,
    sources,
    cross,
    tones,
    parts,
    parts_in,
    stats,
    stats_in,
    own,
    mixed_out,
    chip,
    landed,
    tone_part,
    tone_chip,
    tone_landed,
    load,
    plane_send,
    plane_recv,
    tone_send,
    tone_recv,
    square_send,
    square_recv,
    key_send,
    key_recv,
    query_send,
    query_recv,
    back_send,
    back_recv,
    late_send,
    late_recv,
    side_send,
    side_recv,
    hop_send,
    hop_recv,
    tone_out_send,
    tone_out_recv,
):
    ctx = lax.axis_index("ctx")
    me = lax.axis_index("head")
    rows, width = video_ref.shape
    audio_rows, audio_width = audio_ref.shape
    count = rows // CHUNK
    local_heads = width // HD
    cross_width = w_cross.shape[2]
    cross_heads = cross_width // HD
    peer = [head_peer(me, flip) for flip in range(8)]
    mates = [(ctx + d) % ctx_size for d in range(ctx_size)]
    others = range(1, ctx_size)

    def loader(slot, source, target):
        return pltpu.make_async_copy(source, target, load.at[slot])

    loads = [
        loader(0, w_self_ref.at[1], w_self.at[1]),
        loader(1, w_self_ref.at[2], w_self.at[2]),
        loader(2, w_self_ref.at[0], w_self.at[0]),
        loader(3, w_cross_ref, w_cross),
        loader(4, w_audio_ref, w_audio),
        loader(5, w_out_ref, w_out),
        loader(6, w_cross_out_ref, w_cross_out),
        loader(7, w_audio_out_ref, w_audio_out),
    ]
    for one in loads:
        one.start()

    barrier = pltpu.get_barrier_semaphore()
    friends = [(ctx, peer[flip]) for flip in range(1, 8)]
    friends += [(mates[d], me) for d in others]
    for friend in friends:
        pl.semaphore_signal(barrier, inc=1, device_id=friend, device_id_type=MESH)

    def at_rows(k):
        return aligned(k * CHUNK, CHUNK)

    def columns(block):
        return aligned(block * width, width)

    def tone_columns(block):
        return aligned(block * audio_width, audio_width)

    my_tones = aligned(ctx * audio_rows, audio_rows)

    def scale(k):
        wide = video_ref[pl.ds(k * CHUNK, CHUNK)].astype(F32)
        xs[pl.ds(k * CHUNK, CHUNK), columns(me)] = (wide * video_gain_ref[...]).astype(BF16)
        squares[k : k + 1] = to_row(jnp.sum(wide * wide, axis=1, keepdims=True))

    scale(0)
    raw[my_tones] = audio_ref[...]
    pl.semaphore_wait(barrier, len(friends))

    def hop(slot, k):
        flip, block = (slot, me) if slot in (1, 2, 4, 6) else (1, peer[slot - 1])
        part = xs.at[at_rows(k), columns(block)]
        return remote(
            part, part, plane_send.at[slot - 1, k], plane_recv.at[slot - 1, k], (ctx, peer[flip])
        )

    def tone_hop(slot):
        flip, block = (slot, me) if slot in (1, 2, 4, 6) else (1, peer[slot - 1])
        part = xa.at[:, tone_columns(block)]
        return remote(
            part, part, tone_send.at[slot - 1], tone_recv.at[slot - 1], (ctx, peer[flip])
        )

    def square_hop(kind, flip):
        source, target = (
            (tone_squares, every_tone_square) if kind else (squares, every_square)
        )
        return remote(
            source,
            target.at[flip],
            square_send.at[kind, flip - 1],
            square_recv.at[kind, flip - 1],
            (ctx, peer[flip]),
        )

    def late_copy(kind, d):
        source, target = {
            0: (audio_ref, raw.at[my_tones]),
            1: (parts.at[mates[d]], parts_in.at[ctx]),
            2: (stats.at[mates[d]], stats_in.at[ctx]),
        }[kind]
        return remote(
            source, target, late_send.at[kind, d - 1], late_recv.at[kind, d - 1], (mates[d], me)
        )

    def key_copy(k, d):
        return remote(
            heads.at[mates[d], pl.ds(1, 2), at_rows(k)],
            sources.at[ctx, pl.ds(1, 2), at_rows(k)],
            key_send.at[d - 1, k],
            key_recv.at[d - 1, k],
            (mates[d], me),
        )

    def query_copy(k, d):
        return remote(
            heads.at[mates[d], 0, at_rows(k)],
            sources.at[ctx, 0, at_rows(k)],
            query_send.at[d - 1, k],
            query_recv.at[d - 1, k],
            (mates[d], me),
        )

    for slot in (6, 2, 4, 1):
        hop(slot, 0).start()
    for d in others:
        late_copy(0, d).start()
    for k in range(1, count):
        scale(k)
    every_square[0] = squares[...]
    for flip in range(1, 8):
        square_hop(0, flip).start()

    def begin(k, carry):
        for slot in (6, 2, 4, 1):
            hop(slot, k).start()
        return carry

    lax.fori_loop(1, count, begin, 0)

    for d in others:
        late_copy(0, d).wait_recv()
    tone_squares[...] = jnp.zeros_like(tone_squares)
    for d in range(ctx_size):
        at = pl.ds(d * audio_rows, audio_rows)
        wide = raw[at].astype(F32)
        xa[at, tone_columns(me)] = (wide * audio_gain_ref[...]).astype(BF16)
        tone_squares[d : d + 1] = to_row(jnp.sum(wide * wide, axis=1, keepdims=True))
    every_tone_square[0] = tone_squares[...]
    for one in loads[:4]:
        one.wait()
    for flip in range(1, 8):
        square_hop(0, flip).wait_recv()
    for flip in range(1, 8):
        square_hop(1, flip).start()
    for slot in (6, 2, 4, 1):
        tone_hop(slot).start()

    def video_rate(k):
        sums = jnp.sum(every_square[:, pl.ds(k, 1), :], axis=0)
        return to_column(lax.rsqrt(sums / (8 * width) + EPSILON), CHUNK)

    def cross_project(k):
        at = at_rows(k)
        rate = video_rate(k)

        def one(plane, carry):
            acc = jnp.dot(xs[at, :], w_cross[plane], preferred_element_type=F32)
            scaled = (acc * rate).astype(BF16)
            for h in range(cross_heads):
                cross[h, plane, at] = scaled[:, h * HD : (h + 1) * HD]
            return carry

        lax.fori_loop(0, 3, one, 0)

    def ship(k):
        for d in others:
            query_copy(k, d).start()

    def project(k, carry):
        at = at_rows(k)
        for slot in (2, 4, 6):
            hop(slot, k).wait_recv()
            hop(slot + 1, k).start()

        @pl.when(k > 0)
        def _():
            cross_project(k - 1)

        for slot in (1, 3, 5, 7):
            hop(slot, k).wait_recv()
        rate = video_rate(k)

        def one(i, carry):
            plane = (i + 1) % 3
            acc = jnp.dot(xs[at, :], w_self[plane], preferred_element_type=F32)
            scaled = (acc * rate).astype(BF16)
            for h in range(local_heads):
                heads[h, plane, at] = scaled[:, h * HD : (h + 1) * HD]

            @pl.when(i == 1)
            def _():
                for d in others:
                    key_copy(k, d).start()

            return carry

        lax.fori_loop(0, 3, one, 0)

        @pl.when(k == count - 2)
        def _():
            ship(0)

        for plane in range(3):
            sources[ctx, plane, at] = heads[ctx, plane, at]
        return carry

    lax.fori_loop(0, count, project, 0)

    ship(1)
    cross_project(count - 1)


    def tone_project():
        for slot in (2, 4, 6):
            tone_hop(slot).wait_recv()
            tone_hop(slot + 1).start()
        loads[4].wait()
        for flip in range(1, 8):
            square_hop(1, flip).wait_recv()
        for slot in (1, 3, 5, 7):
            tone_hop(slot).wait_recv()
        tone_sums = jnp.sum(every_tone_square[...], axis=0)
        tone_rates = lax.rsqrt(tone_sums / (8 * audio_width) + EPSILON)
        rate = jnp.concatenate(
            [to_column(tone_rates[d : d + 1], audio_rows) for d in range(ctx_size)], axis=0
        )
        for plane in range(3):
            acc = jnp.dot(xa[...], w_audio[plane], preferred_element_type=F32)
            tones[:, plane * cross_width : (plane + 1) * cross_width] = (acc * rate).astype(BF16)

    def tone_part_of(plane, h):
        return slice(plane * cross_width + h * HD, plane * cross_width + (h + 1) * HD)

    def answer():
        for h in range(cross_heads):
            lanes = slice(h * HD, (h + 1) * HD)

            def one(d, carry):
                query = tones[aligned(d * audio_rows, audio_rows), tone_part_of(0, h)]
                mixed, total, highest = softmax_parts(query, [cross[h, 1]], [cross[h, 2]])
                parts[d, :, lanes] = (mixed / total).astype(BF16)
                stats[d, 2 * h : 2 * h + 1] = to_row(total)
                stats[d, 2 * h + 1 : 2 * h + 2] = to_row(highest)
                return carry

            lax.fori_loop(0, ctx_size, one, 0)
        for d in others:
            late_copy(1, d).start()
            late_copy(2, d).start()
        parts_in[ctx] = parts[ctx]
        stats_in[ctx] = stats[ctx]

    def ask(k):
        at = at_rows(k)
        pieces = []
        for h in range(cross_heads):
            mixed, total, _ = softmax_parts(
                cross[h, 0, at], [tones[:, tone_part_of(1, h)]], [tones[:, tone_part_of(2, h)]]
            )
            pieces.append((mixed / total).astype(BF16))
        return jnp.concatenate(pieces, axis=1)

    def settle_hops(k, carry):
        for slot in range(1, 8):
            hop(slot, k).wait_send()
        for d in others:
            key_copy(k, d).wait_recv()
        return carry

    lax.fori_loop(0, count, settle_hops, 0)
    for one in loads[5:]:
        one.wait()
    ones = jnp.ones((rows, HD), BF16)
    for s in range(ctx_size):
        w_self[0, s * rows : (s + 1) * rows, :HD] = sources[s, 2]
        w_self[0, s * rows : (s + 1) * rows, HD : 2 * HD] = ones

    def reducer(part_at, chip, landed, at, side_sems, hop_sems, out_ref, base_ref):
        def side(i):
            return remote(
                part_at(peer[2 * i + 1]), chip.at[i, at], *side_sems(i), (ctx, peer[1])
            )

        def hop(i):
            return remote(
                chip.at[i, at], landed.at[i - 1, at], *hop_sems(i - 1), (ctx, peer[2 * i])
            )

        def start():
            for i in (3, 1, 2, 0):
                side(i).start()

        def join():
            for i in (3, 1, 2):
                side(i).wait_recv()
                chip[i, at] = (
                    chip[i, at].astype(F32) + part_at(peer[2 * i])[...].astype(F32)
                ).astype(BF16)
                hop(i).start()

        def close():
            side(0).wait_recv()
            total = chip[0, at].astype(F32) + part_at(me)[...].astype(F32)
            total = total + base_ref[at].astype(F32)
            for i in (1, 2, 3):
                hop(i).wait_recv()
                total = total + landed[i - 1, at].astype(F32)
            out_ref[at] = total.astype(BF16)

        def settle():
            for i in range(4):
                side(i).wait_send()
            for i in (1, 2, 3):
                hop(i).wait_send()

        return start, join, close, settle

    def video_steps(k):
        return reducer(
            lambda block: xs.at[at_rows(k), columns(block)],
            chip,
            landed,
            at_rows(k),
            lambda i: (side_send.at[i, k], side_recv.at[i, k]),
            lambda slot: (hop_send.at[slot, k], hop_recv.at[slot, k]),
            video_out_ref,
            video_ref,
        )

    tone_start, tone_join, tone_close, tone_settle = reducer(
        lambda block: tone_part.at[block],
        tone_chip,
        tone_landed,
        pl.ds(0, audio_rows),
        lambda i: (tone_out_send.at[i], tone_out_recv.at[i]),
        lambda slot: (tone_out_send.at[4 + slot], tone_out_recv.at[4 + slot]),
        audio_out_ref,
        audio_ref,
    )

    def sound():
        for d in others:
            late_copy(1, d).wait_recv()
            late_copy(2, d).wait_recv()
        pieces = []
        for h in range(cross_heads):
            lanes = slice(h * HD, (h + 1) * HD)
            totals = [stats_in[s, 2 * h : 2 * h + 1] for s in range(ctx_size)]
            highs = [stats_in[s, 2 * h + 1 : 2 * h + 2] for s in range(ctx_size)]
            top = functools.reduce(jnp.maximum, highs)
            shares = [total * jnp.exp2(high - top) for total, high in zip(totals, highs)]
            whole = functools.reduce(jnp.add, shares)
            mixed = 0.0
            for s in range(ctx_size):
                share = to_column(shares[s] / whole, audio_rows)
                mixed = mixed + parts_in[s, :, lanes].astype(F32) * share
            pieces.append(mixed.astype(BF16))
        result = jnp.concatenate(pieces, axis=1)
        for n in range(8):
            tone_part[n] = jnp.dot(
                result,
                w_audio_out[:, n * audio_width : (n + 1) * audio_width],
                preferred_element_type=F32,
            ).astype(BF16)
        tone_start()

    def back(k, d):
        return remote(
            own.at[mates[d], at_rows(k)],
            mixed_out.at[ctx, at_rows(k)],
            back_send.at[d - 1, k],
            back_recv.at[d - 1, k],
            (mates[d], me),
        )

    def attend_pair(k, first):
        at = at_rows(k)
        pair = [mates[(first + i) % ctx_size] for i in range(2)]
        query = jnp.concatenate([sources[s, 0, at] for s in pair], axis=0)
        scores = [contract_last(query, sources[s, 1]) for s in range(ctx_size)]
        highest = jnp.max(scores[0], axis=1, keepdims=True)
        mixed = None
        for s in range(ctx_size):
            if s:
                higher = jnp.maximum(highest, jnp.max(scores[s], axis=1, keepdims=True))
                fade = jnp.exp2((highest - higher) * SCORE_SCALE)
                highest = higher
            weight = jnp.exp2((scores[s] - highest) * SCORE_SCALE).astype(BF16)
            step = jnp.dot(
                weight,
                w_self[0, s * rows : (s + 1) * rows, : 2 * HD],
                preferred_element_type=F32,
            )
            mixed = mixed * fade + step if s else step
        done = (mixed[:, :HD] / mixed[:, HD:]).astype(BF16)
        for i, s in enumerate(pair):
            own[s, at] = done[i * CHUNK : (i + 1) * CHUNK]
            d = (first + i) % ctx_size
            if d:
                back(k, d).start()
            else:
                mixed_out[ctx, at] = done[i * CHUNK : (i + 1) * CHUNK]

    def output(k):
        at = at_rows(k)
        for d in others:
            back(k, d).wait_recv()
        selfs = jnp.concatenate([mixed_out[s, at] for s in range(ctx_size)], axis=1)
        crossed = ask(k)

        def one(n, carry):
            cols = columns(n)
            xs[at, cols] = (
                jnp.dot(selfs, w_out[:, cols], preferred_element_type=F32)
                + jnp.dot(crossed, w_cross_out[:, cols], preferred_element_type=F32)
            ).astype(BF16)
            return carry

        lax.fori_loop(0, 8, one, 0, unroll=2)
        video_steps(k)[0]()

    def turn(k, carry):
        for d in others:
            query_copy(k, d).wait_recv()
        attend_pair(k, 1)

        @pl.when(k >= 2)
        def _():
            video_steps(k - 2)[1]()

        attend_pair(k, 3)

        @pl.when(k + 2 < count)
        def _():
            ship(k + 2)

        @pl.when(k >= 1)
        def _():
            output(k - 1)

        @pl.when(k >= 4)
        def _():
            video_steps(k - 4)[2]()

        for step, work in ((0, tone_project), (4, answer), (5, sound), (5, tone_join)):
            pl.when(k == step)(work)
        return carry

    lax.fori_loop(0, count, turn, 0)
    last = count - 1
    video_steps(last - 1)[1]()
    video_steps(last - 3)[2]()
    output(last)
    tone_close()
    video_steps(last - 2)[2]()
    video_steps(last)[1]()
    video_steps(last - 1)[2]()
    video_steps(last)[2]()

    def finish(k, carry):
        for d in others:
            key_copy(k, d).wait_send()
            query_copy(k, d).wait_send()
            back(k, d).wait_send()
        video_steps(k)[3]()
        return carry

    lax.fori_loop(0, count, finish, 0)
    for d in others:
        for kind in range(3):
            late_copy(kind, d).wait_send()
    for slot in range(1, 8):
        tone_hop(slot).wait_send()
    for flip in range(1, 8):
        for kind in range(2):
            square_hop(kind, flip).wait_send()
    tone_settle()


def fast_body(
    ctx_size,
    video,
    audio,
    video_gain,
    audio_gain,
    video_qkv,
    video_cross,
    audio_cross,
    video_out,
    cross_video_out,
    cross_audio_out,
):
    rows, width = video.shape
    audio_rows, audio_width = audio.shape
    depth = video_qkv.shape[0]
    audio_depth = audio_cross.shape[0]
    cross_width = video_cross.shape[2]
    count = rows // CHUNK
    cross_heads = cross_width // HD
    lines = (count + 7) // 8 * 8
    others = ctx_size - 1
    every_tone = ctx_size * audio_rows
    vmem = pl.BlockSpec(memory_space=pltpu.VMEM)
    anywhere = pl.BlockSpec(memory_space=pl.ANY)

    def wide(*shape):
        return pltpu.VMEM(shape, BF16)

    def fine(*shape):
        return pltpu.VMEM(shape, F32)

    def pair(*shape):
        return [pltpu.SemaphoreType.DMA(shape)] * 2

    return pl.pallas_call(
        functools.partial(block_kernel, ctx_size),
        out_shape=(
            jax.ShapeDtypeStruct(video.shape, BF16),
            jax.ShapeDtypeStruct(audio.shape, BF16),
        ),
        in_specs=[vmem] * 4 + [anywhere] * 6,
        out_specs=(vmem, vmem),
        scratch_shapes=[
            wide(rows, depth),
            wide(every_tone, audio_depth),
            wide(every_tone, audio_width),
            fine(lines, HD),
            fine(8, lines, HD),
            fine(8, HD),
            fine(8, 8, HD),
            wide(3, depth, width),
            wide(3, depth, cross_width),
            wide(3, audio_depth, cross_width),
            wide(*video_out.shape),
            wide(*cross_video_out.shape),
            wide(*cross_audio_out.shape),
            wide(ctx_size, 3, rows, HD),
            wide(ctx_size, 3, rows, HD),
            wide(cross_heads, 3, rows, HD),
            wide(every_tone, 3 * cross_width),
            wide(ctx_size, audio_rows, cross_width),
            wide(ctx_size, audio_rows, cross_width),
            fine(ctx_size, 8, HD),
            fine(ctx_size, 8, HD),
            wide(ctx_size, rows, HD),
            wide(ctx_size, rows, HD),
            wide(4, rows, width),
            wide(3, rows, width),
            wide(8, audio_rows, audio_width),
            wide(4, audio_rows, audio_width),
            wide(3, audio_rows, audio_width),
            pltpu.SemaphoreType.DMA((8,)),
            *pair(7, count),
            *pair(7),
            *pair(2, 7),
            *pair(others, count),
            *pair(others, count),
            *pair(others, count),
            *pair(3, others),
            *pair(4, count),
            *pair(3, count),
            *pair(7),
        ],
        compiler_params=pltpu.CompilerParams(
            collective_id=0, has_side_effects=True, vmem_limit_bytes=VMEM_LIMIT
        ),
        name="block",
    )(
        video,
        audio,
        video_gain.reshape(1, -1),
        audio_gain.reshape(1, -1),
        video_qkv.transpose(1, 0, 2),
        video_cross.transpose(1, 0, 2),
        audio_cross.transpose(1, 0, 2),
        video_out,
        cross_video_out,
        cross_audio_out,
    )


def suits(ctx_size, head_size, video, audio, video_cross):
    rows, width = video.shape
    audio_rows, audio_width = audio.shape
    return (
        head_size == 8
        and ctx_size == 4
        and width == ctx_size * HD
        and rows % CHUNK == 0
        and rows >= 6 * CHUNK
        and audio_rows % 16 == 0
        and audio_rows <= HD
        and audio_width % HD == 0
        and video_cross.shape[2] % HD == 0
        and video_cross.shape[2] <= 4 * HD
        and ctx_size * rows <= video_cross.shape[0]
    )


def solution(mesh):
    ctx_size = mesh.shape["ctx"]

    def body(*operands):
        if suits(ctx_size, mesh.shape["head"], operands[0], operands[1], operands[5]):
            return fast_body(ctx_size, *operands)
        return plain_body(*operands)

    return jax.shard_map(
        body,
        mesh=mesh,
        in_specs=(
            P("ctx", "head"),
            P("ctx", "head"),
            P("head"),
            P("head"),
            P(None, None, "head"),
            P(None, None, "head"),
            P(None, None, "head"),
            P("head", None),
            P("head", None),
            P("head", None),
        ),
        out_specs=(P("ctx", "head"), P("ctx", "head")),
        check_vma=False,
    )
```
